16 devices in a mesh: data: 2 (over y, z), expert: 8 (over x, core).
Axes of the slice: x: 4, y: 2, z: 1, core: 2. Of those that a mesh axis runs over, the one named last changes fastest.
The devices are a block of a 4x4x8 slice.
Arguments:
- x_tokens: bfloat16 [1024, 1024], P(('data', 'expert')), parts along dimension 0
- y_mid: bfloat16 [1024, 1024], P(('data', 'expert')), parts along dimension 0
- dy_out: bfloat16 [1024, 1024], P(('data', 'expert')), parts along dimension 0
- experts_one: int32 [1024, 8], P(('data', 'expert')), parts along dimension 0
- gates_one: float32 [1024, 8], P(('data', 'expert')), parts along dimension 0
- slots_one: int32 [1024, 8], P(('data', 'expert')), parts along dimension 0
- experts_two: int32 [1024, 8], P(('data', 'expert')), parts along dimension 0
- gates_two: float32 [1024, 8], P(('data', 'expert')), parts along dimension 0
- slots_two: int32 [1024, 8], P(('data', 'expert')), parts along dimension 0
- w_gate_one: bfloat16 [32, 1024, 512], P('expert')
- w_up_one: bfloat16 [32, 1024, 512], P('expert')
- w_down_one: bfloat16 [32, 512, 1024], P('expert')
- w_gate_two: bfloat16 [32, 1024, 512], P('expert')
- w_up_two: bfloat16 [32, 1024, 512], P('expert')
- w_down_two: bfloat16 [32, 512, 1024], P('expert')
Outputs:
- output 1: bfloat16 [1024, 1024], P(('data', 'expert')), parts along dimension 0
- output 2: float32 [64, 1024, 512], P(('data', 'expert')), parts along dimension 0
- output 3: float32 [64, 1024, 512], P(('data', 'expert')), parts along dimension 0
- output 4: float32 [64, 512, 1024], P(('data', 'expert')), parts along dimension 0
- output 5: float32 [64, 1024, 512], P(('data', 'expert')), parts along dimension 0
- output 6: float32 [64, 1024, 512], P(('data', 'expert')), parts along dimension 0
- output 7: float32 [64, 512, 1024], P(('data', 'expert')), parts along dimension 0
There are 2 independent parts. The reference program is written for one: setup_inputs(seed, part) draws one part's arguments, and reference() takes and returns one part's arrays. A program takes and returns all parts, laid end to end along the dimension named above; an argument that names none is the same for every part.
All inputs are finite; a program needn't handle non-finite values.
Results may differ from the reference program's by a relative error of at most 0.01323.
Values are sent between devices in bfloat16 or wider.
A program may use at most 768 MiB of HBM per device.

```python
import jax
import jax.numpy as jnp
from jax import lax

MODEL_DIM = 1024
FFN_DIM = 512
EXPERTS = 32
TOP_K = 8
TOKENS_DEV = 64
GROUP_SIZE = 8

TOKENS_PART = GROUP_SIZE * TOKENS_DEV
CAPACITY = 8 * ((3 * TOP_K * TOKENS_DEV + 16 * EXPERTS - 1) // (16 * EXPERTS))
TOTAL_ROWS = GROUP_SIZE * EXPERTS * CAPACITY


def draw_routing(key):
    key_noise, key_bias, key_hot = jax.random.split(key, 3)
    noise_int = jax.random.randint(key_noise, (TOKENS_PART, EXPERTS), 0, 4096)
    expert_bias = jax.random.randint(key_bias, (EXPERTS,), 0, 512)
    hot_expert = jax.random.randint(key_hot, (), 0, EXPERTS)
    expert_ids = jnp.arange(EXPERTS, dtype=jnp.int32)
    local_tok = jnp.arange(TOKENS_PART, dtype=jnp.int32) % TOKENS_DEV
    boost_int = jnp.where((local_tok[:, None] < CAPACITY) & (expert_ids[None, :] == hot_expert), 8192, 0)
    score_int = (noise_int + expert_bias[None, :] + boost_int) * EXPERTS + expert_ids[None, :]
    top_vals, experts = lax.top_k(score_int, TOP_K)
    flat_ids = experts.reshape(GROUP_SIZE, TOKENS_DEV * TOP_K)
    onehot = (flat_ids[:, :, None] == expert_ids[None, None, :]).astype(jnp.int32)
    slot_rank = jnp.sum((jnp.cumsum(onehot, axis=1) - 1) * onehot, axis=2)
    slots = jnp.where(slot_rank < CAPACITY, slot_rank, -1).reshape(TOKENS_PART, TOP_K)
    return experts.astype(jnp.int32), slots.astype(jnp.int32)


def draw_weight(key, shape, fan_in):
    return (jax.random.normal(key, shape, jnp.float32) * fan_in ** -0.5).astype(jnp.bfloat16)


def setup_inputs(seed: int = 0, part: int = 0) -> dict:
    key_part = jax.random.fold_in(jax.random.key(seed), part)
    keys = jax.random.split(key_part, 7)
    shared = jax.random.split(jax.random.key(seed + 1), 6)
    tok_shape = (TOKENS_PART, MODEL_DIM)
    route_shape = (TOKENS_PART, TOP_K)
    up_shape = (EXPERTS, MODEL_DIM, FFN_DIM)
    down_shape = (EXPERTS, FFN_DIM, MODEL_DIM)
    gate_scale = TOP_K ** -0.5
    experts_one, slots_one = draw_routing(keys[3])
    experts_two, slots_two = draw_routing(keys[4])
    return {
        "x_tokens": jax.random.normal(keys[0], tok_shape, jnp.float32).astype(jnp.bfloat16),
        "y_mid": jax.random.normal(keys[1], tok_shape, jnp.float32).astype(jnp.bfloat16),
        "dy_out": jax.random.normal(keys[2], tok_shape, jnp.float32).astype(jnp.bfloat16),
        "experts_one": experts_one,
        "gates_one": jax.random.uniform(keys[5], route_shape, jnp.float32, 0.5, 1.5) * gate_scale,
        "slots_one": slots_one,
        "experts_two": experts_two,
        "gates_two": jax.random.uniform(keys[6], route_shape, jnp.float32, 0.5, 1.5) * gate_scale,
        "slots_two": slots_two,
        "w_gate_one": draw_weight(shared[0], up_shape, MODEL_DIM),
        "w_up_one": draw_weight(shared[1], up_shape, MODEL_DIM),
        "w_down_one": draw_weight(shared[2], down_shape, FFN_DIM),
        "w_gate_two": draw_weight(shared[3], up_shape, MODEL_DIM),
        "w_up_two": draw_weight(shared[4], up_shape, MODEL_DIM),
        "w_down_two": draw_weight(shared[5], down_shape, FFN_DIM),
    }


def expert_grads(operands):
    x_rows, z_rows, w_gate, w_up, w_down = operands
    gate_act = jnp.dot(x_rows, w_gate, preferred_element_type=jnp.float32).astype(jnp.bfloat16).astype(jnp.float32)
    up_act = jnp.dot(x_rows, w_up, preferred_element_type=jnp.float32).astype(jnp.bfloat16).astype(jnp.float32)
    sig_gate = jax.nn.sigmoid(gate_act)
    silu_gate = gate_act * sig_gate
    hidden = (silu_gate * up_act).astype(jnp.bfloat16)
    d_hidden = jnp.dot(z_rows, w_down.T, preferred_element_type=jnp.float32)
    dw_down = jnp.dot(hidden.T, z_rows, preferred_element_type=jnp.float32)
    d_gate = (d_hidden * up_act * sig_gate * (1.0 + gate_act * (1.0 - sig_gate))).astype(jnp.bfloat16)
    d_up = (d_hidden * silu_gate).astype(jnp.bfloat16)
    dx_rows = (jnp.dot(d_gate, w_gate.T, preferred_element_type=jnp.float32) + jnp.dot(d_up, w_up.T, preferred_element_type=jnp.float32)).astype(jnp.bfloat16)
    dw_gate = jnp.dot(x_rows.T, d_gate, preferred_element_type=jnp.float32)
    dw_up = jnp.dot(x_rows.T, d_up, preferred_element_type=jnp.float32)
    return dx_rows, dw_gate, dw_up, dw_down


def layer_backward(inputs, cotangent, experts, gates, slots, w_gate, w_up, w_down):
    source = jnp.arange(TOKENS_PART, dtype=jnp.int32) // TOKENS_DEV
    target = jnp.where(slots >= 0, (source[:, None] * EXPERTS + experts) * CAPACITY + slots, TOTAL_ROWS).reshape(-1)
    x_copies = jnp.repeat(inputs, TOP_K, axis=0)
    z_copies = (gates[:, :, None] * cotangent[:, None, :].astype(jnp.float32)).astype(jnp.bfloat16).reshape(TOKENS_PART * TOP_K, MODEL_DIM)
    x_buffer = jnp.zeros((TOTAL_ROWS + 1, MODEL_DIM), jnp.bfloat16).at[target].add(x_copies)
    z_buffer = jnp.zeros((TOTAL_ROWS + 1, MODEL_DIM), jnp.bfloat16).at[target].add(z_copies)
    by_source = (GROUP_SIZE, EXPERTS, CAPACITY, MODEL_DIM)
    by_expert = (EXPERTS, GROUP_SIZE * CAPACITY, MODEL_DIM)
    x_rows = x_buffer[:TOTAL_ROWS].reshape(by_source).transpose(1, 0, 2, 3).reshape(by_expert)
    z_rows = z_buffer[:TOTAL_ROWS].reshape(by_source).transpose(1, 0, 2, 3).reshape(by_expert)
    dx_rows, dw_gate, dw_up, dw_down = lax.map(expert_grads, (x_rows, z_rows, w_gate, w_up, w_down))
    returned = dx_rows.reshape(EXPERTS, GROUP_SIZE, CAPACITY, MODEL_DIM).transpose(1, 0, 2, 3).reshape(TOTAL_ROWS, MODEL_DIM)
    returned = jnp.concatenate([returned, jnp.zeros((1, MODEL_DIM), jnp.bfloat16)], axis=0)
    per_copy = returned[target].reshape(TOKENS_PART, TOP_K, MODEL_DIM).astype(jnp.float32)
    return jnp.sum(per_copy, axis=1), dw_gate, dw_up, dw_down


def reference(x_tokens, y_mid, dy_out, experts_one, gates_one, slots_one, experts_two, gates_two, slots_two, w_gate_one, w_up_one, w_down_one, w_gate_two, w_up_two, w_down_two):
    grads_two = layer_backward(y_mid, dy_out, experts_two, gates_two, slots_two, w_gate_two, w_up_two, w_down_two)
    dy_mid = (dy_out.astype(jnp.float32) + grads_two[0]).astype(jnp.bfloat16)
    grads_one = layer_backward(x_tokens, dy_mid, experts_one, gates_one, slots_one, w_gate_one, w_up_one, w_down_one)
    dx_tokens = (dy_mid.astype(jnp.float32) + grads_one[0]).astype(jnp.bfloat16)
    return (dx_tokens, grads_one[1], grads_one[2], grads_one[3], grads_two[1], grads_two[2], grads_two[3])
```

```python
import functools
import jax
import jax.numpy as jnp
from jax import lax
from jax.experimental import pallas as pl
from jax.experimental.pallas import tpu as pltpu
from jax.sharding import PartitionSpec as P

MESH = pl.DeviceIdType.MESH
F32 = jnp.float32
BF16 = jnp.bfloat16
NT = (((1,), (1,)), ((), ()))
TN = (((0,), (0,)), ((), ()))
CHUNKS = 4


def dot(a, b, dims=(((1,), (0,)), ((), ()))):
    return lax.dot_general(a, b, dims, preferred_element_type=F32)


def slot_capacity(tokens_dev, top_k, n_experts):
    return 8 * ((3 * top_k * tokens_dev + 16 * n_experts - 1) // (16 * n_experts))


class Link:
    def __init__(self, send, recv):
        self.send, self.recv, self.used, self.started = send, recv, 0, []

    def copy(self, src, dst, device):
        k = self.used
        self.used += 1
        return pltpu.make_async_remote_copy(
            src_ref=src, dst_ref=dst, send_sem=self.send.at[k], recv_sem=self.recv.at[k],
            device_id={"expert": device}, device_id_type=MESH)

    def start(self, c):
        c.start()
        self.started.append(c)

    def drain(self):
        for c in self.started:
            c.wait_send()


class Gather:
    def __init__(self, link, place, own, buf, split):
        me, partner, left, right, far = place
        self.link = link
        half = own.shape[0] // 2
        a, b = pl.ds(0, half), pl.ds(half, half)
        self.pair = link.copy(own, buf.at[me], partner)
        if split:
            self.first = [link.copy(own.at[a], buf.at[me, a], right), link.copy(own.at[b], buf.at[me, b], left)]
            self.second = [link.copy(own.at[b], buf.at[me, b], right), link.copy(own.at[a], buf.at[me, a], left)]
            self.relay = [link.copy(buf.at[left, a], buf.at[left, a], right), link.copy(buf.at[right, b], buf.at[right, b], left)]
            far_pair = [link.copy(buf.at[far, a], buf.at[far, a], partner), link.copy(buf.at[far, b], buf.at[far, b], partner)]
        else:
            self.first = [link.copy(own, buf.at[me], right), link.copy(own, buf.at[me], left)]
            self.second = []
            self.relay = [link.copy(buf.at[left], buf.at[left], right)]
            far_pair = [link.copy(buf.at[far], buf.at[far], partner)]
        self.near_pair = [link.copy(buf.at[left], buf.at[left], partner), link.copy(buf.at[right], buf.at[right], partner)]
        self.far_pair = far_pair

    def begin(self):
        for c in self.first + self.second + [self.pair]:
            self.link.start(c)

    def forward(self):
        for c in self.first:
            c.wait_recv()
        for c in self.relay:
            self.link.start(c)

    def share_near(self):
        for c in self.second:
            c.wait_recv()
        for c in self.near_pair:
            self.link.start(c)

    def share_far(self):
        for c, d in zip(self.relay, self.far_pair):
            c.wait_recv()
            self.link.start(d)

    def finish(self):
        for c in [self.pair] + self.near_pair + self.far_pair:
            c.wait_recv()


def main_kernel(dims, x_ref, y_ref, dy_ref, rt_ref, wg1, wu1, wd1, wg2, wu2, wd2,
                u2_o, z2_o, h2_o, da2_o, db2_o, u1_o, z1_o, h1_o, da1_o, db1_o, dmid_o, own_o, qr_o, ql_o, qf_o,
                wv, rtg, yg, gg, xg, dg, oh, ot, grow, u, z, act_a, act_b, h, da, db, dxb,
                d1own, q, sd, rd, ra, rb, fl, fr, send, recv, wsem, osem):
    n_dev, tokens, model, ffn, n_local, cap = dims
    n_chips = n_dev // 2
    me = lax.axis_index("expert")
    chip, core = me // 2, lax.rem(me, 2)
    partner = chip * 2 + 1 - core
    right = lax.rem(chip + 1, n_chips) * 2 + core
    left = lax.rem(chip + n_chips - 1, n_chips) * 2 + core
    far = lax.rem(chip + 2, n_chips) * 2 + core
    place = (me, partner, left, right, far)
    rows_chip = 2 * cap
    rows = n_local * rows_chip
    cw = model // CHUNKS
    half = tokens // 2

    wload = []
    for i, w in enumerate((wg2, wu2, wd2, wg1, wu1, wd1)):
        c = pltpu.make_async_copy(w, wv[i], wsem.at[i])
        c.start()
        wload.append(c)

    barrier = pltpu.get_barrier_semaphore()
    for d in (partner, left, right):
        pl.semaphore_signal(barrier, inc=1, device_id={"expert": d}, device_id_type=MESH)
    pl.semaphore_wait(barrier, 3)

    link = Link(send, recv)
    g_rt = Gather(link, place, rt_ref, rtg, False)
    g_y = Gather(link, place, y_ref, yg, True)
    g_g = Gather(link, place, dy_ref, gg, True)
    g_x = Gather(link, place, x_ref, xg, True)
    g_rt.begin()
    g_y.begin()
    g_g.begin()
    rtg[me] = rt_ref[...]
    yg[me] = y_ref[...]
    gg[me] = dy_ref[...]
    xg[me] = x_ref[...]
    g_rt.forward()
    g_rt.share_near()
    g_y.forward()
    g_rt.share_far()
    g_y.share_near()
    g_g.forward()
    g_x.begin()
    g_rt.finish()

    def build(layer):
        lane = lax.broadcasted_iota(jnp.int32, (8, 2 * tokens), 1)
        rid = lax.broadcasted_iota(jnp.int32, (rows, 2 * tokens), 0).astype(F32)
        base = (me * (n_local * rows_chip)).astype(F32)

        def one(c, carry):
            r0, r1 = rtg[2 * c], rtg[2 * c + 1]

            def pick(lo):
                p0, p1 = r0[lo:lo + 8], r1[lo:lo + 8]
                if layer == 0:
                    return jnp.where(lane < tokens, p0, pltpu.roll(p1, tokens, 1))
                return jnp.where(lane < tokens, pltpu.roll(p0, tokens, 1), p1)

            t, g = pick(0) - base, pick(8)
            hit = jnp.zeros((rows, 2 * tokens), F32)
            gm = jnp.zeros((rows, 2 * tokens), F32)
            for j in range(8):
                m = t[j:j + 1] == rid
                hit = jnp.where(m, 1.0, hit)
                gm = jnp.where(m, g[j:j + 1], gm)
            oh[layer, c] = hit.astype(BF16)
            ot[layer, c] = hit.T.astype(BF16)
            grow[layer, c] = jnp.sum(gm, axis=1, keepdims=True)
            return carry

        lax.fori_loop(0, n_chips, one, 0)

    def rows_of(layer, buf, dst, gated, cols=None):
        lo, width = (0, model) if cols is None else cols

        def one(c, carry):
            src = jnp.concatenate([buf[2 * c], buf[2 * c + 1]], axis=0)
            r = dot(oh[layer, c], src)
            if gated:
                r = r * grow[layer, c]
            r = r.astype(BF16)
            for e in range(n_local):
                dst[layer, e, pl.ds(pl.multiple_of(c * rows_chip, 16), rows_chip), lo:lo + width] = r[e * rows_chip:(e + 1) * rows_chip]
            return carry

        lax.fori_loop(0, n_chips, one, 0)

    def forward_act(layer, e):
        ue = u[layer, e]
        a = dot(ue, wv[3 * layer][e]).astype(BF16)
        b = dot(ue, wv[3 * layer + 1][e]).astype(BF16)
        aw, bw = a.astype(F32), b.astype(F32)
        act_a[e] = a
        act_b[e] = b
        h[layer, e] = (aw * jax.nn.sigmoid(aw) * bw).astype(BF16)

    def back_act(layer, e):
        dh = dot(z[layer, e], wv[3 * layer + 2][e], NT)
        aw, bw = act_a[e].astype(F32), act_b[e].astype(F32)
        sig = jax.nn.sigmoid(aw)
        da[layer, e] = (dh * bw * sig * (1.0 + aw * (1.0 - sig))).astype(BF16)
        db[layer, e] = (dh * (aw * sig)).astype(BF16)

    def each_expert(fn):
        def body(e, carry):
            fn(e)
            return carry
        lax.fori_loop(0, n_local, body, 0)

    outs = []

    def put(src, dst):
        c = pltpu.make_async_copy(src, dst, osem.at[len(outs)])
        c.start()
        outs.append(c)

    def dx_chunk(layer, k):
        cols = slice(k * cw, (k + 1) * cw)

        def one(e):
            d = dot(da[layer, e], wv[3 * layer][e, cols], NT) + dot(db[layer, e], wv[3 * layer + 1][e, cols], NT)
            d = d.astype(BF16)
            for c in range(n_chips):
                dxb[c, pl.ds(pl.multiple_of(e * rows_chip, 16), rows_chip)] = d[c * rows_chip:(c + 1) * rows_chip]

        each_expert(one)

        def comb(c, carry):
            q_all[c] = dot(ot[layer, c], dxb[c])
            return carry

        q_all = q.at[layer, k]
        lax.fori_loop(0, n_chips, comb, 0)

    build(0)
    g_y.share_far()
    g_y.finish()
    g_g.share_near()
    rows_of(0, yg, u, False)
    put(u.at[0], u2_o)
    wload[0].wait()
    wload[1].wait()
    g_g.share_far()
    g_x.forward()
    each_expert(lambda e: forward_act(0, e))
    put(h.at[0], h2_o)
    g_g.finish()
    g_x.share_near()
    rows_of(0, gg, z, True)
    put(z.at[0], z2_o)
    wload[2].wait()
    each_expert(lambda e: back_act(0, e))
    put(da.at[0], da2_o)
    put(db.at[0], db2_o)
    g_x.share_far()

    mine, theirs = pl.multiple_of(core * tokens, tokens), pl.multiple_of((1 - core) * tokens, tokens)

    pair = {}
    for layer in range(2):
        for k in range(CHUNKS):
            pair[layer, k] = link.copy(q.at[layer, k, :, pl.ds(theirs, tokens)], rd.at[layer, k], partner)
    qs = [sd.at[k] for k in range(CHUNKS)]
    rs_far = [[link.copy(qs[k].at[far // 2, pl.ds(0, half)], ra.at[k], right),
               link.copy(qs[k].at[far // 2, pl.ds(half, half)], rb.at[k], left)] for k in range(CHUNKS)]
    rs_near = [[link.copy(qs[k].at[right // 2], fl.at[k], right),
                link.copy(qs[k].at[left // 2], fr.at[k], left)] for k in range(CHUNKS)]
    ag = [Gather(link, place, d1own.at[k], dg.at[k], True) for k in range(CHUNKS)]

    def stage_far(k):
        pair[0, k].wait_recv()
        sd[k] = q[0, k, :, pl.ds(mine, tokens)] + rd[0, k]
        for c in rs_far[k]:
            link.start(c)

    def stage_near(k):
        for c in rs_far[k]:
            c.wait_recv()
        sd[k, right // 2, 0:half] = sd[k, right // 2, 0:half] + ra[k]
        sd[k, left // 2, half:] = sd[k, left // 2, half:] + rb[k]
        for c in rs_near[k]:
            link.start(c)

    def stage_sum(k):
        for c in rs_near[k]:
            c.wait_recv()
        total = sd[k, chip] + (fl[k] + fr[k])
        d = (dy_ref[:, k * cw:(k + 1) * cw].astype(F32) + total).astype(BF16)
        d1own[k] = d
        dg[k, me] = d
        ag[k].begin()

    for k in range(CHUNKS):
        dx_chunk(0, k)
        link.start(pair[0, k])
        if k >= 1:
            stage_far(k - 1)
        if k >= 2:
            stage_near(k - 2)
    stage_far(CHUNKS - 1)
    build(1)
    g_x.finish()
    rows_of(1, xg, u, False)
    put(u.at[1], u1_o)
    wload[3].wait()
    wload[4].wait()
    stage_near(CHUNKS - 2)
    forward_act(1, 0)
    stage_near(CHUNKS - 1)
    stage_sum(0)
    forward_act(1, 1)
    stage_sum(1)
    ag[0].forward()
    forward_act(1, 2)
    stage_sum(2)
    ag[0].share_near()
    ag[1].forward()
    forward_act(1, 3)
    put(h.at[1], h1_o)
    stage_sum(3)
    ag[0].share_far()
    ag[1].share_near()
    ag[2].forward()
    ag[1].share_far()
    ag[2].share_near()
    ag[3].forward()
    ag[2].share_far()
    ag[3].share_near()
    wload[5].wait()
    for k in range(CHUNKS):
        if k == CHUNKS - 1:
            ag[k].share_far()
        ag[k].finish()
        rows_of(1, dg.at[k], z, True, (k * cw, cw))
    put(z.at[1], z1_o)

    each_expert(lambda e: back_act(1, e))
    put(da.at[1], da1_o)
    put(db.at[1], db1_o)

    def stage_out(k):
        pair[1, k].wait_recv()
        cols = slice(k * cw, (k + 1) * cw)
        for c, o in ((chip, own_o), (right // 2, qr_o), (left // 2, ql_o), (far // 2, qf_o)):
            o[:, cols] = q[1, k, c, pl.ds(mine, tokens)] + rd[1, k, c]
        dmid_o[:, cols] = d1own[k]

    for k in range(CHUNKS):
        dx_chunk(1, k)
        link.start(pair[1, k])
        if k >= 1:
            stage_out(k - 1)
    stage_out(CHUNKS - 1)

    link.drain()
    for c in outs:
        c.wait()


def grad_kernel(n_local, *refs):
    ins, outs = refs[:10], refs[10:16]
    vin, vout, isem, osem = refs[16:]
    loads = []
    for i, r in enumerate(ins):
        c = pltpu.make_async_copy(r, vin[i], isem.at[i])
        c.start()
        loads.append(c)

    def stores(layer, e, s):
        return [pltpu.make_async_copy(vout[i].at[s], outs[3 * layer + i].at[e], osem.at[i, s]) for i in range(3)]

    for layer in range(2):
        for c in loads[5 * layer:5 * layer + 5]:
            c.wait()
        u, z, h, da, db = vin[5 * layer:5 * layer + 5]

        def body(e, carry, layer=layer, u=u, z=z, h=h, da=da, db=db):
            s = lax.rem(e, 2)

            def reclaim():
                for c in stores(layer, e, s):
                    c.wait()

            if layer == 0:
                pl.when(e >= 2)(reclaim)
            else:
                reclaim()
            vout[0][s] = dot(u[e], da[e], TN)
            vout[1][s] = dot(u[e], db[e], TN)
            vout[2][s] = dot(h[e], z[e], TN)
            for c in stores(layer, e, s):
                c.start()
            return carry

        lax.fori_loop(0, n_local, body, 0)
    for s in range(2):
        for c in stores(1, n_local - 2 + s, s):
            c.wait()


def solution(mesh):
    n_dev = mesh.shape["expert"]
    tok_spec = P(("data", "expert"), None)
    weight_spec = P("expert", None, None)
    grad_spec = P(("data", "expert"), None, None)

    def local_step(x, y, dy, experts_one, gates_one, slots_one, experts_two, gates_two, slots_two, wg1, wu1, wd1, wg2, wu2, wd2):
        tokens, model = x.shape
        n_local, _, ffn = wg1.shape
        top_k = experts_one.shape[1]
        cap = slot_capacity(tokens, top_k, n_local * n_dev)
        n_chips = n_dev // 2
        rows = n_local * 2 * cap
        cw = model // CHUNKS
        half = tokens // 2
        core = lax.rem(lax.axis_index("expert"), 2)

        def target(experts, slots):
            return jnp.where(slots >= 0, experts * (2 * cap) + core * cap + slots, -1).astype(F32)

        rt = jnp.concatenate([
            jnp.concatenate([target(experts_two, slots_two), gates_two], axis=1),
            jnp.concatenate([target(experts_one, slots_one), gates_one], axis=1)], axis=0).T

        S = jax.ShapeDtypeStruct
        er = n_chips * 2 * cap
        wide, narrow = S((n_local, er, model), BF16), S((n_local, er, ffn), BF16)
        saved = [wide, wide, narrow, narrow, narrow]
        part = S((tokens, model), F32)
        hbm, vm = pl.BlockSpec(memory_space=pl.ANY), pl.BlockSpec(memory_space=pltpu.VMEM)
        V = pltpu.VMEM
        scratch = [
            [V(w.shape, BF16) for w in (wg2, wu2, wd2, wg1, wu1, wd1)],
            V((n_dev,) + rt.shape, F32),
            V((n_dev, tokens, model), BF16), V((n_dev, tokens, model), BF16), V((n_dev, tokens, model), BF16),
            V((CHUNKS, n_dev, tokens, cw), BF16),
            V((2, n_chips, rows, 2 * tokens), BF16), V((2, n_chips, 2 * tokens, rows), BF16), V((2, n_chips, rows, 1), F32),
            V((2, n_local, er, model), BF16), V((2, n_local, er, model), BF16),
            V((n_local, er, ffn), BF16), V((n_local, er, ffn), BF16),
            V((2, n_local, er, ffn), BF16), V((2, n_local, er, ffn), BF16), V((2, n_local, er, ffn), BF16),
            V((n_chips, rows, cw), BF16),
            V((CHUNKS, tokens, cw), BF16),
            V((2, CHUNKS, n_chips, 2 * tokens, cw), F32),
            V((CHUNKS, n_chips, tokens, cw), F32),
            V((2, CHUNKS, n_chips, tokens, cw), F32),
            V((CHUNKS, half, cw), F32), V((CHUNKS, half, cw), F32),
            V((CHUNKS, tokens, cw), F32), V((CHUNKS, tokens, cw), F32),
            pltpu.SemaphoreType.DMA((128,)), pltpu.SemaphoreType.DMA((128,)),
            pltpu.SemaphoreType.DMA((6,)), pltpu.SemaphoreType.DMA((10,)),
        ]
        res = pl.pallas_call(
            functools.partial(main_kernel, (n_dev, tokens, model, ffn, n_local, cap)),
            out_shape=saved + saved + [S((tokens, model), BF16)] + [part] * 4,
            in_specs=[vm] * 4 + [hbm] * 6,
            out_specs=[hbm] * 10 + [vm] * 5,
            scratch_shapes=scratch,
            compiler_params=pltpu.CompilerParams(collective_id=0, has_side_effects=True, vmem_limit_bytes=62 * 2**20),
            name="moe_main",
        )(x, y, dy, rt, wg1, wu1, wd1, wg2, wu2, wd2)
        kept2, kept1 = res[:5], res[5:10]
        dmid, own, q_right, q_left, q_far = res[10:]

        def shift(v, by):
            return lax.ppermute(v, "expert", [(i, (i + by) % n_dev) for i in range(n_dev)])

        from_left, from_right, from_far = shift(q_right, 2), shift(q_left, n_dev - 2), shift(q_far, n_dev // 2)

        up, down = S((n_local, model, ffn), F32), S((n_local, ffn, model), F32)
        flops = 2 * 2 * n_local * er * model * ffn * 3
        grads = pl.pallas_call(
            functools.partial(grad_kernel, n_local),
            out_shape=[up, up, down] * 2,
            in_specs=[hbm] * 10,
            out_specs=[hbm] * 6,
            scratch_shapes=[
                [V(s.shape, BF16) for s in saved + saved],
                [V((2, model, ffn), F32), V((2, model, ffn), F32), V((2, ffn, model), F32)],
                pltpu.SemaphoreType.DMA((10,)), pltpu.SemaphoreType.DMA((3, 2))],
            compiler_params=pltpu.CompilerParams(vmem_limit_bytes=48 * 2**20),
            cost_estimate=pl.CostEstimate(flops=flops, bytes_accessed=6 * n_local * model * ffn * 4, transcendentals=0),
            name="moe_grads",
        )(*kept2, *kept1)
        dx = (dmid.astype(F32) + ((own + from_far) + (from_left + from_right))).astype(BF16)
        return (dx,) + tuple(grads[3:]) + tuple(grads[:3])

    return jax.shard_map(local_step, mesh=mesh, in_specs=(tok_spec,) * 9 + (weight_spec,) * 6, out_specs=(tok_spec,) + (grad_spec,) * 6, check_vma=False)
```

```python
import functools
import jax
import jax.numpy as jnp
from jax import lax
from jax.experimental import pallas as pl
from jax.experimental.pallas import tpu as pltpu
from jax.sharding import PartitionSpec as P

MESH = pl.DeviceIdType.MESH
F32 = jnp.float32
BF16 = jnp.bfloat16
NT = (((1,), (1,)), ((), ()))
TN = (((0,), (0,)), ((), ()))
CHUNKS = 4
MAIN_VMEM = 44 * 2**20
GRAD_VMEM = 24 * 2**20


def dot(a, b, dims=(((1,), (0,)), ((), ()))):
    return lax.dot_general(a, b, dims, preferred_element_type=F32)


def slot_capacity(tokens_dev, top_k, n_experts):
    return 8 * ((3 * top_k * tokens_dev + 16 * n_experts - 1) // (16 * n_experts))


def scoped(name):
    def deco(fn):
        def run(*args, **kw):
            with jax.named_scope(name):
                return fn(*args, **kw)
        return run
    return deco


class Link:
    def __init__(self, send, recv):
        self.send, self.recv, self.used, self.started = send, recv, 0, []

    def copy(self, src, dst, device):
        k = self.used
        self.used += 1
        return pltpu.make_async_remote_copy(
            src_ref=src, dst_ref=dst, send_sem=self.send.at[k], recv_sem=self.recv.at[k],
            device_id={"expert": device}, device_id_type=MESH)

    def start(self, c):
        c.start()
        self.started.append(c)

    @scoped("drain")
    def drain(self):
        for c in self.started:
            c.wait_send()


class Gather:
    def __init__(self, link, place, own, buf, split):
        me, partner, left, right, far = place
        self.link = link
        half = own.shape[0] // 2
        a, b = pl.ds(0, half), pl.ds(half, half)
        self.pair = link.copy(own, buf.at[me], partner)
        if split:
            self.first = [link.copy(own.at[a], buf.at[me, a], right), link.copy(own.at[b], buf.at[me, b], left)]
            self.second = [link.copy(own.at[b], buf.at[me, b], right), link.copy(own.at[a], buf.at[me, a], left)]
            self.relay = [link.copy(buf.at[left, a], buf.at[left, a], right), link.copy(buf.at[right, b], buf.at[right, b], left)]
            far_pair = [link.copy(buf.at[far, a], buf.at[far, a], partner), link.copy(buf.at[far, b], buf.at[far, b], partner)]
        else:
            self.first = [link.copy(own, buf.at[me], right), link.copy(own, buf.at[me], left)]
            self.second = []
            self.relay = [link.copy(buf.at[left], buf.at[left], right)]
            far_pair = [link.copy(buf.at[far], buf.at[far], partner)]
        self.near_pair = [link.copy(buf.at[left], buf.at[left], partner), link.copy(buf.at[right], buf.at[right], partner)]
        self.far_pair = far_pair

    @scoped("ag_begin")
    def begin(self):
        for c in self.first + self.second + [self.pair]:
            self.link.start(c)

    @scoped("ag_forward")
    def forward(self):
        for c in self.first:
            c.wait_recv()
        for c in self.relay:
            self.link.start(c)

    @scoped("ag_share_near")
    def share_near(self):
        for c in self.second:
            c.wait_recv()
        for c in self.near_pair:
            self.link.start(c)

    @scoped("ag_share_far")
    def share_far(self):
        for c, d in zip(self.relay, self.far_pair):
            c.wait_recv()
            self.link.start(d)

    @scoped("ag_finish")
    def finish(self):
        for c in [self.pair] + self.near_pair + self.far_pair:
            c.wait_recv()


def main_kernel(dims, x_ref, y_ref, dy_ref, e1, g1, s1, e2, g2, s2, wg1, wu1, wd1, wg2, wu2, wd2,
                saved, own_o, dmid_o, qr_o, ql_o, qf_o,
                wv, rt, rtg, yg, gg, xg, dg, oh, ot, grow, act_a, act_b, dxb,
                d1own, q, sd, rd, ra, rb, fl, fr, send, recv, wsem, osem):
    n_dev, tokens, model, ffn, n_local, cap = dims
    n_chips = n_dev // 2
    me = lax.axis_index("expert")
    chip, core = me // 2, lax.rem(me, 2)
    partner = chip * 2 + 1 - core
    right = lax.rem(chip + 1, n_chips) * 2 + core
    left = lax.rem(chip + n_chips - 1, n_chips) * 2 + core
    far = lax.rem(chip + 2, n_chips) * 2 + core
    place = (me, partner, left, right, far)
    rows_chip = 2 * cap
    rows = n_local * rows_chip
    cw = model // CHUNKS
    half = tokens // 2
    u, z, h, da, db = ([saved[i], saved[5 + i]] for i in range(5))

    barrier = pltpu.get_barrier_semaphore()
    for d in (partner, left, right):
        pl.semaphore_signal(barrier, inc=1, device_id={"expert": d}, device_id_type=MESH)

    wload = []
    for i, w in enumerate((wg2, wu2, wd2, wg1, wu1, wd1)):
        c = pltpu.make_async_copy(w, wv[i], wsem.at[i])
        c.start()
        wload.append(c)

    def target(experts, slots):
        return jnp.where(slots >= 0, experts * rows_chip + core * cap + slots, -1).astype(F32)

    top_k = e1.shape[0]
    rt[0:top_k, 0:tokens] = target(e2[...], s2[...])
    rt[0:top_k, tokens:2 * tokens] = target(e1[...], s1[...])
    rt[top_k:2 * top_k, 0:tokens] = g2[...]
    rt[top_k:2 * top_k, tokens:2 * tokens] = g1[...]

    link = Link(send, recv)
    g_rt = Gather(link, place, rt, rtg, False)
    g_y = Gather(link, place, y_ref, yg, True)
    g_g = Gather(link, place, dy_ref, gg, True)
    g_x = Gather(link, place, x_ref, xg, True)
    rtg[me] = rt[...]
    yg[me] = y_ref[...]
    gg[me] = dy_ref[...]
    xg[me] = x_ref[...]

    with jax.named_scope("barrier"):
        pl.semaphore_wait(barrier, 3)

    @scoped("build")
    def build(layer):
        lane = lax.broadcasted_iota(jnp.int32, (top_k, 2 * tokens), 1)
        rid = lax.broadcasted_iota(jnp.int32, (rows, 2 * tokens), 0).astype(F32)
        base = (me * (n_local * rows_chip)).astype(F32)

        def one(c, carry):
            r0, r1 = rtg[2 * c], rtg[2 * c + 1]

            def pick(lo):
                p0, p1 = r0[lo:lo + top_k], r1[lo:lo + top_k]
                if layer == 0:
                    return jnp.where(lane < tokens, p0, pltpu.roll(p1, tokens, 1))
                return jnp.where(lane < tokens, pltpu.roll(p0, tokens, 1), p1)

            t, g = pick(0) - base, pick(top_k)
            hit = jnp.zeros((rows, 2 * tokens), F32)
            gm = jnp.zeros((rows, 2 * tokens), F32)
            for j in range(top_k):
                m = t[j:j + 1] == rid
                hit = jnp.where(m, 1.0, hit)
                gm = jnp.where(m, g[j:j + 1], gm)
            oh[layer, c] = hit.astype(BF16)
            ot[layer, c] = hit.T.astype(BF16)
            grow[layer, c] = jnp.sum(gm, axis=1, keepdims=True)
            return carry

        lax.fori_loop(0, n_chips, one, 0)

    @scoped("rows_of")
    def rows_of(layer, buf, dst, gated, cols=None):
        lo, width = (0, model) if cols is None else cols
        for c in range(n_chips):
            src = jnp.concatenate([buf[2 * c], buf[2 * c + 1]], axis=0)
            r = dot(oh[layer, c], src)
            if gated:
                r = r * grow[layer, c]
            r = r.astype(BF16)
            for e in range(n_local):
                dst[e, c * rows_chip:(c + 1) * rows_chip, lo:lo + width] = r[e * rows_chip:(e + 1) * rows_chip]

    @scoped("forward_act")
    def forward_act(layer, e):
        ue = u[layer][e]
        a = dot(ue, wv[3 * layer][e]).astype(BF16)
        b = dot(ue, wv[3 * layer + 1][e]).astype(BF16)
        aw, bw = a.astype(F32), b.astype(F32)
        act_a[e] = a
        act_b[e] = b
        h[layer][e] = (aw * jax.nn.sigmoid(aw) * bw).astype(BF16)

    @scoped("back_act")
    def back_act(layer, e):
        dh = dot(z[layer][e], wv[3 * layer + 2][e], NT)
        aw, bw = act_a[e].astype(F32), act_b[e].astype(F32)
        sig = jax.nn.sigmoid(aw)
        da[layer][e] = (dh * bw * sig * (1.0 + aw * (1.0 - sig))).astype(BF16)
        db[layer][e] = (dh * (aw * sig)).astype(BF16)

    def each_expert(fn):
        def body(e, carry):
            fn(e)
            return carry
        lax.fori_loop(0, n_local, body, 0)

    outs = []

    def put(src, dst):
        c = pltpu.make_async_copy(src, dst, osem.at[len(outs)])
        c.start()
        outs.append(c)

    @scoped("dx_chunk")
    def dx_chunk(layer, k):
        cols = slice(k * cw, (k + 1) * cw)
        for e in range(n_local):
            d = dot(da[layer][e], wv[3 * layer][e, cols], NT) + dot(db[layer][e], wv[3 * layer + 1][e, cols], NT)
            d = d.astype(BF16)
            for c in range(n_chips):
                dxb[k, c, e * rows_chip:(e + 1) * rows_chip] = d[c * rows_chip:(c + 1) * rows_chip]
        for c in range(n_chips):
            q[layer, k, c] = dot(ot[layer, c], dxb[k, c])

    mine, theirs = pl.multiple_of(core * tokens, tokens), pl.multiple_of((1 - core) * tokens, tokens)

    pair = {}
    for layer in range(2):
        for k in range(CHUNKS):
            pair[layer, k] = link.copy(q.at[layer, k, :, pl.ds(theirs, tokens)], rd.at[layer, k], partner)
    rs_far = [[link.copy(sd.at[k, far // 2, pl.ds(0, half)], ra.at[k], right),
               link.copy(sd.at[k, far // 2, pl.ds(half, half)], rb.at[k], left)] for k in range(CHUNKS)]
    rs_near = [[link.copy(sd.at[k, right // 2], fl.at[k], right),
                link.copy(sd.at[k, left // 2], fr.at[k], left)] for k in range(CHUNKS)]
    ag = [Gather(link, place, d1own.at[k], dg.at[k], True) for k in range(CHUNKS)]

    @scoped("stage_far")
    def stage_far(k):
        pair[0, k].wait_recv()
        sd[k] = q[0, k, :, pl.ds(mine, tokens)] + rd[0, k]
        for c in rs_far[k]:
            link.start(c)

    @scoped("stage_near")
    def stage_near(k):
        for c in rs_far[k]:
            c.wait_recv()
        sd[k, right // 2, 0:half] = sd[k, right // 2, 0:half] + ra[k]
        sd[k, left // 2, half:] = sd[k, left // 2, half:] + rb[k]
        for c in rs_near[k]:
            link.start(c)

    @scoped("stage_sum")
    def stage_sum(k):
        for c in rs_near[k]:
            c.wait_recv()
        total = sd[k, chip] + (fl[k] + fr[k])
        d = (dy_ref[:, k * cw:(k + 1) * cw].astype(F32) + total).astype(BF16)
        d1own[k] = d
        dg[k, me] = d
        dmid_o[:, k * cw:(k + 1) * cw] = d
        ag[k].begin()

    @scoped("stage_out")
    def stage_out(k):
        pair[1, k].wait_recv()
        cols = slice(k * cw, (k + 1) * cw)
        own_o[:, cols] = q[1, k, chip, pl.ds(mine, tokens)] + rd[1, k, chip]
        for c, o in ((right // 2, qr_o), (left // 2, ql_o), (far // 2, qf_o)):
            rd[1, k, c] = q[1, k, c, pl.ds(mine, tokens)] + rd[1, k, c]
            put(rd.at[1, k, c], o.at[:, pl.ds(k * cw, cw)])

    def z_chunk(k):
        ag[k].finish()
        rows_of(1, dg.at[k], z[1], True, (k * cw, cw))

    g_rt.begin()
    g_y.begin()
    g_rt.forward()
    g_rt.share_near()
    g_y.forward()
    g_g.begin()
    g_rt.share_far()
    g_y.share_near()
    g_rt.finish()
    build(0)
    g_y.share_far()
    g_g.forward()
    g_x.begin()
    g_y.finish()
    rows_of(0, yg, u[0], False)
    g_g.share_near()
    wload[0].wait()
    wload[1].wait()
    forward_act(0, 0)
    forward_act(0, 1)
    g_g.share_far()
    forward_act(0, 2)
    forward_act(0, 3)
    g_g.finish()
    rows_of(0, gg, z[0], True)
    wload[2].wait()
    each_expert(lambda e: back_act(0, e))

    for k in range(CHUNKS):
        dx_chunk(0, k)
        link.start(pair[0, k])
        if k >= 2:
            stage_far(k - 2)
        if k == 0:
            g_x.forward()
            g_x.share_near()
    stage_far(CHUNKS - 2)
    g_x.share_far()
    stage_far(CHUNKS - 1)
    build(1)
    stage_near(0)
    stage_near(1)
    g_x.finish()
    rows_of(1, xg, u[1], False)
    stage_near(2)
    stage_near(3)
    wload[3].wait()
    wload[4].wait()
    forward_act(1, 0)
    stage_sum(0)
    forward_act(1, 1)
    stage_sum(1)
    ag[0].forward()
    forward_act(1, 2)
    ag[0].share_near()
    stage_sum(2)
    ag[1].forward()
    forward_act(1, 3)
    ag[0].share_far()
    ag[1].share_near()
    stage_sum(3)
    ag[2].forward()
    ag[1].share_far()
    ag[2].share_near()
    z_chunk(0)
    ag[3].forward()
    ag[2].share_far()
    ag[3].share_near()
    z_chunk(1)
    ag[3].share_far()
    z_chunk(2)
    z_chunk(3)
    wload[5].wait()

    each_expert(lambda e: back_act(1, e))
    for k in range(CHUNKS):
        dx_chunk(1, k)
        link.start(pair[1, k])
        if k >= 2:
            stage_out(k - 2)
    stage_out(CHUNKS - 2)
    stage_out(CHUNKS - 1)

    link.drain()
    for c in outs:
        c.wait()


def grad_kernel(n_local, *refs):
    ins, outs = refs[:10], refs[10:16]
    vout, osem = refs[16:]

    def stores(layer, e, s):
        return [pltpu.make_async_copy(vout[i].at[s], outs[3 * layer + i].at[e], osem.at[i, s]) for i in range(3)]

    for layer in range(2):
        u, z, h, da, db = ins[5 * layer:5 * layer + 5]

        def body(e, carry, layer=layer, u=u, z=z, h=h, da=da, db=db):
            s = lax.rem(e, 2)
            for i, (a, b) in enumerate(((u, da), (u, db), (h, z))):
                def reclaim(i=i):
                    stores(layer, e, s)[i].wait()

                if layer == 0:
                    pl.when(e >= 2)(reclaim)
                else:
                    reclaim()
                vout[i][s] = dot(a[e], b[e], TN)
                stores(layer, e, s)[i].start()
            return carry

        lax.fori_loop(0, n_local, body, 0)
    for s in range(2):
        for c in stores(1, n_local - 2 + s, s):
            c.wait()


def solution(mesh):
    n_dev = mesh.shape["expert"]
    tok_spec = P(("data", "expert"), None)
    weight_spec = P("expert", None, None)
    grad_spec = P(("data", "expert"), None, None)

    def local_step(x, y, dy, experts_one, gates_one, slots_one, experts_two, gates_two, slots_two, wg1, wu1, wd1, wg2, wu2, wd2):
        tokens, model = x.shape
        n_local, _, ffn = wg1.shape
        top_k = experts_one.shape[1]
        cap = slot_capacity(tokens, top_k, n_local * n_dev)
        n_chips = n_dev // 2
        rows = n_local * 2 * cap
        cw = model // CHUNKS
        half = tokens // 2

        S = jax.ShapeDtypeStruct
        er = n_chips * 2 * cap
        wide, narrow = S((n_local, er, model), BF16), S((n_local, er, ffn), BF16)
        saved = [wide, wide, narrow, narrow, narrow]
        part = S((tokens, model), F32)
        hbm, vm = pl.BlockSpec(memory_space=pltpu.HBM), pl.BlockSpec(memory_space=pltpu.VMEM)
        V = pltpu.VMEM
        scratch = [
            [V(w.shape, BF16) for w in (wg2, wu2, wd2, wg1, wu1, wd1)],
            V((2 * top_k, 2 * tokens), F32), V((n_dev, 2 * top_k, 2 * tokens), F32),
            V((n_dev, tokens, model), BF16), V((n_dev, tokens, model), BF16), V((n_dev, tokens, model), BF16),
            V((CHUNKS, n_dev, tokens, cw), BF16),
            V((2, n_chips, rows, 2 * tokens), BF16), V((2, n_chips, 2 * tokens, rows), BF16), V((2, n_chips, rows, 1), F32),
            V((n_local, er, ffn), BF16), V((n_local, er, ffn), BF16),
            V((CHUNKS, n_chips, rows, cw), BF16),
            V((CHUNKS, tokens, cw), BF16),
            V((2, CHUNKS, n_chips, 2 * tokens, cw), F32),
            V((CHUNKS, n_chips, tokens, cw), F32),
            V((2, CHUNKS, n_chips, tokens, cw), F32),
            V((CHUNKS, half, cw), F32), V((CHUNKS, half, cw), F32),
            V((CHUNKS, tokens, cw), F32), V((CHUNKS, tokens, cw), F32),
            pltpu.SemaphoreType.DMA((128,)), pltpu.SemaphoreType.DMA((128,)),
            pltpu.SemaphoreType.DMA((6,)), pltpu.SemaphoreType.DMA((3 * CHUNKS,)),
        ]
        kept, own, dmid, q_right, q_left, q_far = pl.pallas_call(
            functools.partial(main_kernel, (n_dev, tokens, model, ffn, n_local, cap)),
            out_shape=[[V(s.shape, s.dtype) for s in saved + saved], part, S((tokens, model), BF16), part, part, part],
            in_specs=[vm] * 9 + [hbm] * 6,
            out_specs=[[vm] * 10, vm, vm, hbm, hbm, hbm],
            scratch_shapes=scratch,
            compiler_params=pltpu.CompilerParams(collective_id=0, has_side_effects=True, vmem_limit_bytes=MAIN_VMEM),
            name="moe_main",
        )(x, y, dy, experts_one.T, gates_one.T, slots_one.T, experts_two.T, gates_two.T, slots_two.T, wg1, wu1, wd1, wg2, wu2, wd2)

        def shift(v, by):
            return lax.ppermute(v, "expert", [(i, (i + by) % n_dev) for i in range(n_dev)])

        from_left, from_right, from_far = shift(q_right, 2), shift(q_left, n_dev - 2), shift(q_far, n_dev // 2)

        up, down = S((n_local, model, ffn), F32), S((n_local, ffn, model), F32)
        flops = 2 * 2 * n_local * er * model * ffn * 3
        grads = pl.pallas_call(
            functools.partial(grad_kernel, n_local),
            out_shape=[up, up, down] * 2,
            in_specs=[vm] * 10,
            out_specs=[hbm] * 6,
            scratch_shapes=[
                [V((2, model, ffn), F32), V((2, model, ffn), F32), V((2, ffn, model), F32)],
                pltpu.SemaphoreType.DMA((3, 2))],
            compiler_params=pltpu.CompilerParams(vmem_limit_bytes=GRAD_VMEM),
            cost_estimate=pl.CostEstimate(flops=flops, bytes_accessed=6 * n_local * model * ffn * 4, transcendentals=0),
            name="moe_grads",
        )(*kept)
        dx = (dmid.astype(F32) + ((own + from_far) + (from_left + from_right))).astype(BF16)
        return (dx,) + tuple(grads[3:]) + tuple(grads[:3])

    return jax.shard_map(local_step, mesh=mesh, in_specs=(tok_spec,) * 9 + (weight_spec,) * 6, out_specs=(tok_spec,) + (grad_spec,) * 6, check_vma=False)
```

```python
import functools
import jax
import jax.numpy as jnp
from jax import lax
from jax.experimental import pallas as pl
from jax.experimental.pallas import tpu as pltpu
from jax.sharding import PartitionSpec as P

MESH = pl.DeviceIdType.MESH
F32 = jnp.float32
BF16 = jnp.bfloat16
NT = (((1,), (1,)), ((), ()))
TN = (((0,), (0,)), ((), ()))
CHUNKS = 4
DIRECT = 2
COPIES = 70
MAIN_VMEM = 50 * 2**20
GRAD_VMEM = 24 * 2**20


def dot(a, b, dims=(((1,), (0,)), ((), ()))):
    return lax.dot_general(a, b, dims, preferred_element_type=F32)


def slot_capacity(tokens_dev, top_k, n_experts):
    return 8 * ((3 * top_k * tokens_dev + 16 * n_experts - 1) // (16 * n_experts))


def scoped(name):
    def deco(fn):
        def run(*args, **kw):
            tag = "_".join([name] + [str(getattr(a, "tag", a)) for a in args if isinstance(a, (int, Gather))])
            with jax.named_scope(tag):
                return fn(*args, **kw)
        return run
    return deco


class Link:
    def __init__(self, send, recv):
        self.send, self.recv, self.used, self.pending = send, recv, 0, {}

    def copy(self, src, dst, device):
        k = self.used
        self.used += 1
        c = pltpu.make_async_remote_copy(
            src_ref=src, dst_ref=dst, send_sem=self.send.at[k], recv_sem=self.recv.at[k],
            device_id={"expert": device}, device_id_type=MESH)
        return k, c

    def start(self, kc):
        k, c = kc
        if k in self.pending:
            self.pending[k].wait_send()
        c.start()
        self.pending[k] = c

    @scoped("drain")
    def drain(self):
        for c in self.pending.values():
            c.wait_send()


class Gather:
    def __init__(self, link, place, own, buf, split, tag, direct=False):
        me, partner, left, right, far = place
        self.link, self.tag, self.direct = link, tag, direct
        half = own.shape[0] // 2
        a, b = pl.ds(0, half), pl.ds(half, half)
        self.pair = link.copy(own, buf.at[me], partner)
        if direct:
            self.first = [link.copy(own, buf.at[me], right), link.copy(own, buf.at[me], left)]
            self.second = []
            self.relay = [link.copy(own, buf.at[me], far)]
            far_pair = [link.copy(buf.at[far], buf.at[far], partner)]
        elif split:
            self.first = [link.copy(own.at[a], buf.at[me, a], right), link.copy(own.at[b], buf.at[me, b], left)]
            self.second = [link.copy(own.at[b], buf.at[me, b], right), link.copy(own.at[a], buf.at[me, a], left)]
            self.relay = [link.copy(buf.at[left, a], buf.at[left, a], right), link.copy(buf.at[right, b], buf.at[right, b], left)]
            far_pair = [link.copy(buf.at[far], buf.at[far], partner)]
        else:
            self.first = [link.copy(own, buf.at[me], right), link.copy(own, buf.at[me], left)]
            self.second = []
            self.relay = [link.copy(buf.at[left], buf.at[left], right)]
            far_pair = [link.copy(buf.at[far], buf.at[far], partner)]
        self.near_pair = [link.copy(buf.at[left], buf.at[left], partner), link.copy(buf.at[right], buf.at[right], partner)]
        self.far_pair = far_pair

    @scoped("ag_begin_first")
    def begin_first(self):
        for c in self.first:
            self.link.start(c)

    @scoped("ag_begin")
    def begin(self, first=True):
        for c in (self.relay if self.direct else []) + (self.first if first else []) + self.second + [self.pair]:
            self.link.start(c)

    @scoped("ag_forward")
    def forward(self):
        for c in self.first:
            c[1].wait_recv()
        for c in [] if self.direct else self.relay:
            self.link.start(c)

    @scoped("ag_share_near")
    def share_near(self):
        for c in self.second:
            c[1].wait_recv()
        for c in self.near_pair:
            self.link.start(c)

    @scoped("ag_share_far")
    def share_far(self):
        for c in self.relay:
            c[1].wait_recv()
        for c in self.far_pair:
            self.link.start(c)

    @scoped("ag_finish")
    def finish(self):
        for c in [self.pair] + self.near_pair + self.far_pair:
            c[1].wait_recv()


def main_kernel(dims, x_in, y_in, dy_in, e1_in, g1_in, s1_in, e2_in, g2_in, s2_in, wg1, wu1, wd1, wg2, wu2, wd2,
                saved, own_o, dmid_o, qr_o, ql_o, qf_o,
                tok, route, gate, wv, rt, rtg, yg, gg, xg, dg, oh, ot, grow, act_a, act_b, dhp, dxb,
                d1own, q, sd, rd, ra, rb, fl, fr, send, recv, isem, wsem):
    n_dev, tokens, model, ffn, n_local, cap = dims
    n_chips = n_dev // 2
    me = lax.axis_index("expert")
    chip, core = me // 2, lax.rem(me, 2)
    partner = chip * 2 + 1 - core
    right = lax.rem(chip + 1, n_chips) * 2 + core
    left = lax.rem(chip + n_chips - 1, n_chips) * 2 + core
    far = lax.rem(chip + 2, n_chips) * 2 + core
    place = (me, partner, left, right, far)
    rows_chip = 2 * cap
    rows = n_local * rows_chip
    cw = model // CHUNKS
    half = tokens // 2
    u, z, h, da, db = ([saved[i], saved[5 + i]] for i in range(5))

    barrier = pltpu.get_barrier_semaphore()
    for d in (partner, left, right, far):
        pl.semaphore_signal(barrier, inc=1, device_id={"expert": d}, device_id_type=MESH)

    x_ref, y_ref, dy_ref = tok
    hw = model // 2
    e1, s1, e2, s2 = route
    g1, g2 = gate
    loads = []
    for i, (r, v) in enumerate(((e1_in, e1), (g1_in, g1), (s1_in, s1), (e2_in, e2), (g2_in, g2), (s2_in, s2), (y_in, y_ref), (x_in, x_ref), (dy_in.at[:, 0:hw], dy_ref.at[0]), (dy_in.at[:, hw:], dy_ref.at[1]))):
        c = pltpu.make_async_copy(r, v, isem.at[i])
        c.start()
        loads.append(c)
    for c in loads[:7]:
        c.wait()

    wload = []
    for i, w in enumerate((wg2, wu2, wd2, wg1, wu1, wd1)):
        c = pltpu.make_async_copy(w, wv[i], wsem.at[i])
        c.start()
        wload.append(c)

    def target(experts, slots):
        return jnp.where(slots >= 0, experts * rows_chip + core * cap + slots, -1).astype(F32)

    top_k = e1.shape[0]
    rt[0:top_k, 0:tokens] = target(e2[...], s2[...])
    rt[0:top_k, tokens:2 * tokens] = target(e1[...], s1[...])
    rt[top_k:2 * top_k, 0:tokens] = g2[...]
    rt[top_k:2 * top_k, tokens:2 * tokens] = g1[...]

    link = Link(send, recv)
    g_rt = Gather(link, place, rt, rtg, False, "rt")
    g_y = Gather(link, place, y_ref, yg, True, "y")
    g_g = [Gather(link, place, dy_ref.at[i], gg.at[i], True, f"g{i}") for i in range(2)]
    g_x = Gather(link, place, x_ref, xg, True, "x")
    rtg[me] = rt[...]
    yg[me] = y_ref[...]
    for c in loads[7:]:
        c.wait()
    for i in range(2):
        gg[i, me] = dy_ref[i]
    xg[me] = x_ref[...]

    with jax.named_scope("barrier"):
        pl.semaphore_wait(barrier, 4)

    @scoped("build")
    def build(layer):
        lane = lax.broadcasted_iota(jnp.int32, (top_k, 2 * tokens), 1)
        rid = lax.broadcasted_iota(jnp.int32, (rows, 2 * tokens), 0).astype(F32)
        base = (me * (n_local * rows_chip)).astype(F32)

        def one(c, carry):
            r0, r1 = rtg[2 * c], rtg[2 * c + 1]

            def pick(lo):
                p0, p1 = r0[lo:lo + top_k], r1[lo:lo + top_k]
                if layer == 0:
                    return jnp.where(lane < tokens, p0, pltpu.roll(p1, tokens, 1))
                return jnp.where(lane < tokens, pltpu.roll(p0, tokens, 1), p1)

            t, g = pick(0) - base, pick(top_k)
            hit = jnp.zeros((rows, 2 * tokens), F32)
            gm = jnp.zeros((rows, 2 * tokens), F32)
            for j in range(top_k):
                m = t[j:j + 1] == rid
                hit = jnp.where(m, 1.0, hit)
                gm = jnp.where(m, g[j:j + 1], gm)
            oh[layer, c] = hit.astype(BF16)
            ot[layer, c] = hit.T.astype(BF16)
            grow[layer, c] = jnp.sum(gm, axis=1, keepdims=True)
            return carry

        lax.fori_loop(0, n_chips, one, 0)

    @scoped("rows_of")
    def rows_of(layer, buf, dst, gated, cols=None):
        lo, width = (0, model) if cols is None else cols
        for c in range(n_chips):
            src = jnp.concatenate([buf[2 * c], buf[2 * c + 1]], axis=0)
            r = dot(oh[layer, c], src)
            if gated:
                r = r * grow[layer, c]
            r = r.astype(BF16)
            for e in range(n_local):
                dst[e, c * rows_chip:(c + 1) * rows_chip, lo:lo + width] = r[e * rows_chip:(e + 1) * rows_chip]

    @scoped("forward_act")
    def forward_act(layer, e):
        ue = u[layer][e]
        aw = dot(ue, wv[3 * layer][e]).astype(BF16).astype(F32)
        bw = dot(ue, wv[3 * layer + 1][e]).astype(BF16).astype(F32)
        sig = jax.nn.sigmoid(aw)
        silu = aw * sig
        h[layer][e] = (silu * bw).astype(BF16)
        act_a[e] = bw * sig * (1.0 + aw * (1.0 - sig))
        act_b[e] = silu

    @scoped("back_part")
    def back_part(layer, e, lo, width):
        part = dot(z[layer][e, :, lo:lo + width], wv[3 * layer + 2][e, :, lo:lo + width], NT)
        dhp[e] = part if lo == 0 else dhp[e] + part

    @scoped("back_act")
    def back_act(layer, e, lo):
        dh = dot(z[layer][e, :, lo:], wv[3 * layer + 2][e, :, lo:], NT)
        if lo:
            dh = dh + dhp[e]
        da[layer][e] = (dh * act_a[e]).astype(BF16)
        db[layer][e] = (dh * act_b[e]).astype(BF16)

    def each_expert(fn):
        def body(e, carry):
            fn(e)
            return carry
        lax.fori_loop(0, n_local, body, 0)

    @scoped("dx_chunk")
    def dx_chunk(layer, k):
        cols = slice(k * cw, (k + 1) * cw)
        for e in range(n_local):
            d = dot(da[layer][e], wv[3 * layer][e, cols], NT) + dot(db[layer][e], wv[3 * layer + 1][e, cols], NT)
            d = d.astype(BF16)
            for c in range(n_chips):
                dxb[k, c, e * rows_chip:(e + 1) * rows_chip] = d[c * rows_chip:(c + 1) * rows_chip]
        for c in range(n_chips):
            q[layer, k, c] = dot(ot[layer, c], dxb[k, c])

    mine, theirs = pl.multiple_of(core * tokens, tokens), pl.multiple_of((1 - core) * tokens, tokens)

    pair, base = {}, link.used
    for layer in range(2):
        link.used = base
        for k in range(CHUNKS):
            pair[layer, k] = link.copy(q.at[layer, k, :, pl.ds(theirs, tokens)], rd.at[layer, k], partner)
    rs_far = [[link.copy(sd.at[k, far // 2, pl.ds(0, half)], ra.at[k], right),
               link.copy(sd.at[k, far // 2, pl.ds(half, half)], rb.at[k], left)] for k in range(CHUNKS)]
    rs_near = [[link.copy(sd.at[k, right // 2], fl.at[k], right),
                link.copy(sd.at[k, left // 2], fr.at[k], left)] for k in range(CHUNKS)]
    link.used = 0
    ag = [Gather(link, place, d1own.at[k], dg.at[k], True, k, direct=k >= CHUNKS - DIRECT) for k in range(CHUNKS)]

    @scoped("stage_far")
    def stage_far(k):
        pair[0, k][1].wait_recv()
        sd[k] = q[0, k, :, pl.ds(mine, tokens)] + rd[0, k]
        for c in rs_far[k]:
            link.start(c)

    @scoped("stage_near")
    def stage_near(k):
        for c in rs_far[k]:
            c[1].wait_recv()
        sd[k, right // 2, 0:half] = sd[k, right // 2, 0:half] + ra[k]
        sd[k, left // 2, half:] = sd[k, left // 2, half:] + rb[k]
        for c in rs_near[k]:
            link.start(c)

    @scoped("stage_sum")
    def stage_sum(k):
        for c in rs_near[k]:
            c[1].wait_recv()
        total = sd[k, chip] + (fl[k] + fr[k])
        d = (dy_ref[k * cw // hw, :, k * cw % hw:k * cw % hw + cw].astype(F32) + total).astype(BF16)
        d1own[k] = d
        dg[k, me] = d
        dmid_o[:, k * cw:(k + 1) * cw] = d
        ag[k].begin()

    @scoped("stage_out")
    def stage_out(k):
        pair[1, k][1].wait_recv()
        cols = slice(k * cw, (k + 1) * cw)
        for c, o in ((chip, own_o), (right // 2, qr_o), (left // 2, ql_o), (far // 2, qf_o)):
            o[:, cols] = q[1, k, c, pl.ds(mine, tokens)] + rd[1, k, c]

    def z_chunk(k):
        ag[k].finish()
        rows_of(1, dg.at[k], z[1], True, (k * cw, cw))

    g_rt.begin()
    g_y.begin()
    g_g[0].begin()
    g_rt.forward()
    g_rt.share_near()
    g_y.forward()
    g_g[1].begin()
    g_rt.share_far()
    g_y.share_near()
    g_rt.finish()
    build(0)
    g_y.share_far()
    g_g[0].forward()
    g_g[1].forward()
    g_x.begin()
    g_y.finish()
    rows_of(0, yg, u[0], False)
    g_g[0].share_near()
    g_g[1].share_near()
    with jax.named_scope("wload"):
        wload[0].wait()
        wload[1].wait()
    forward_act(0, 0)
    build(1)
    g_g[0].share_far()
    forward_act(0, 1)
    forward_act(0, 2)
    g_g[1].share_far()
    forward_act(0, 3)
    g_g[0].finish()
    rows_of(0, gg.at[0], z[0], True, (0, hw))
    with jax.named_scope("wload"):
        wload[2].wait()
    g_g[1].finish()
    rows_of(0, gg.at[1], z[0], True, (hw, hw))
    each_expert(lambda e: back_act(0, e, 0))
    g_x.forward()

    for k in range(CHUNKS):
        dx_chunk(0, k)
        link.start(pair[0, k])
        if k == 0:
            g_x.share_near()
        if k >= 1:
            stage_far(k - 1)
    stage_far(CHUNKS - 1)
    g_x.share_far()
    stage_near(0)
    stage_near(1)
    g_x.finish()
    rows_of(1, xg, u[1], False)
    stage_near(2)
    with jax.named_scope("wload"):
        wload[3].wait()
        wload[4].wait()
    forward_act(1, 0)
    stage_near(3)
    stage_sum(0)
    forward_act(1, 1)
    stage_sum(1)
    forward_act(1, 2)
    stage_sum(2)
    ag[0].forward()
    stage_sum(3)
    ag[1].forward()
    ag[0].share_near()
    ag[1].share_near()
    ag[2].forward()
    ag[0].share_far()
    ag[3].forward()
    ag[2].share_near()
    ag[1].share_far()
    ag[3].share_near()
    forward_act(1, 3)
    with jax.named_scope("wload"):
        wload[5].wait()
    ag[2].share_far()
    z_chunk(0)
    z_chunk(1)
    ag[3].share_far()
    each_expert(lambda e: back_part(1, e, 0, hw))
    z_chunk(2)
    z_chunk(3)

    each_expert(lambda e: back_act(1, e, hw))
    for k in range(CHUNKS):
        dx_chunk(1, k)
        link.start(pair[1, k])
        if k >= 2:
            stage_out(k - 2)
    stage_out(CHUNKS - 2)
    stage_out(CHUNKS - 1)

    link.drain()


def grad_kernel(n_local, *refs):
    ins, outs = refs[:10], refs[10:16]
    vout, osem = refs[16:]

    def store(i, layer, e, s):
        return pltpu.make_async_copy(vout[i].at[s], outs[3 * layer + i].at[e], osem.at[i, s])

    for layer in range(2):
        u, z, h, da, db = ins[5 * layer:5 * layer + 5]

        def body(e, carry, layer=layer, u=u, z=z, h=h, da=da, db=db):
            s = lax.rem(e, 2)
            for i, (a, b) in enumerate(((u, da), (u, db), (h, z))):
                def reclaim(i=i):
                    store(i, layer, e, s).wait()

                if layer == 0:
                    pl.when(e >= 2)(reclaim)
                else:
                    reclaim()
                vout[i][s] = dot(a[e], b[e], TN)
                store(i, layer, e, s).start()
            return carry

        lax.fori_loop(0, n_local, body, 0)
    for s in range(2):
        for i in range(3):
            store(i, 1, n_local - 2 + s, s).wait()


def solution(mesh):
    n_dev = mesh.shape["expert"]
    tok_spec = P(("data", "expert"), None)
    weight_spec = P("expert", None, None)
    grad_spec = P(("data", "expert"), None, None)

    def local_step(x, y, dy, experts_one, gates_one, slots_one, experts_two, gates_two, slots_two, wg1, wu1, wd1, wg2, wu2, wd2):
        tokens, model = x.shape
        n_local, _, ffn = wg1.shape
        top_k = experts_one.shape[1]
        cap = slot_capacity(tokens, top_k, n_local * n_dev)
        n_chips = n_dev // 2
        rows = n_local * 2 * cap
        cw = model // CHUNKS
        half = tokens // 2

        S = jax.ShapeDtypeStruct
        er = n_chips * 2 * cap
        wide, narrow = S((n_local, er, model), BF16), S((n_local, er, ffn), BF16)
        saved = [wide, wide, narrow, narrow, narrow]
        part = S((tokens, model), F32)
        hbm, vm = pl.BlockSpec(memory_space=pltpu.HBM), pl.BlockSpec(memory_space=pltpu.VMEM)
        V = pltpu.VMEM
        scratch = [
            [V((tokens, model), BF16), V((tokens, model), BF16), V((2, tokens, model // 2), BF16)], [V((top_k, tokens), jnp.int32)] * 4, [V((top_k, tokens), F32)] * 2,
            [V(w.shape, BF16) for w in (wg2, wu2, wd2, wg1, wu1, wd1)],
            V((2 * top_k, 2 * tokens), F32), V((n_dev, 2 * top_k, 2 * tokens), F32),
            V((n_dev, tokens, model), BF16), V((2, n_dev, tokens, model // 2), BF16), V((n_dev, tokens, model), BF16),
            V((CHUNKS, n_dev, tokens, cw), BF16),
            V((2, n_chips, rows, 2 * tokens), BF16), V((2, n_chips, 2 * tokens, rows), BF16), V((2, n_chips, rows, 1), F32),
            V((n_local, er, ffn), F32), V((n_local, er, ffn), F32), V((n_local, er, ffn), F32),
            V((CHUNKS, n_chips, rows, cw), BF16),
            V((CHUNKS, tokens, cw), BF16),
            V((2, CHUNKS, n_chips, 2 * tokens, cw), F32),
            V((CHUNKS, n_chips, tokens, cw), F32),
            V((2, CHUNKS, n_chips, tokens, cw), F32),
            V((CHUNKS, half, cw), F32), V((CHUNKS, half, cw), F32),
            V((CHUNKS, tokens, cw), F32), V((CHUNKS, tokens, cw), F32),
            pltpu.SemaphoreType.DMA((COPIES,)), pltpu.SemaphoreType.DMA((COPIES,)),
            pltpu.SemaphoreType.DMA((10,)), pltpu.SemaphoreType.DMA((6,)),
        ]
        kept, own, dmid, q_right, q_left, q_far = pl.pallas_call(
            functools.partial(main_kernel, (n_dev, tokens, model, ffn, n_local, cap)),
            out_shape=[[V(s.shape, s.dtype) for s in saved + saved], V(part.shape, F32), V(part.shape, BF16)] + [V(part.shape, F32)] * 3,
            in_specs=[hbm] * 15,
            out_specs=[[vm] * 10, vm, vm, vm, vm, vm],
            scratch_shapes=scratch,
            compiler_params=pltpu.CompilerParams(collective_id=0, has_side_effects=True, vmem_limit_bytes=MAIN_VMEM),
            name="moe_main",
        )(x, y, dy, experts_one.T, gates_one.T, slots_one.T, experts_two.T, gates_two.T, slots_two.T, wg1, wu1, wd1, wg2, wu2, wd2)

        def shift(v, by):
            return lax.ppermute(v, "expert", [(i, (i + by) % n_dev) for i in range(n_dev)])

        from_left, from_right, from_far = shift(q_right, 2), shift(q_left, n_dev - 2), shift(q_far, n_dev // 2)

        up, down = S((n_local, model, ffn), F32), S((n_local, ffn, model), F32)
        flops = 2 * 2 * n_local * er * model * ffn * 3
        grads = pl.pallas_call(
            functools.partial(grad_kernel, n_local),
            out_shape=[up, up, down] * 2,
            in_specs=[vm] * 10,
            out_specs=[hbm] * 6,
            scratch_shapes=[
                [V((2, model, ffn), F32), V((2, model, ffn), F32), V((2, ffn, model), F32)],
                pltpu.SemaphoreType.DMA((3, 2))],
            compiler_params=pltpu.CompilerParams(vmem_limit_bytes=GRAD_VMEM),
            cost_estimate=pl.CostEstimate(flops=flops, bytes_accessed=6 * n_local * model * ffn * 4, transcendentals=0),
            name="moe_grads",
        )(*kept)
        dx = (dmid.astype(F32) + ((own + from_far) + (from_left + from_right))).astype(BF16)
        return (dx,) + tuple(grads[3:]) + tuple(grads[:3])

    return jax.shard_map(local_step, mesh=mesh, in_specs=(tok_spec,) * 9 + (weight_spec,) * 6, out_specs=(tok_spec,) + (grad_spec,) * 6, check_vma=False)
```

```python
import functools
import jax
import jax.numpy as jnp
from jax import lax
from jax.experimental import pallas as pl
from jax.experimental.pallas import tpu as pltpu
from jax.sharding import PartitionSpec as P

MESH = pl.DeviceIdType.MESH
F32 = jnp.float32
BF16 = jnp.bfloat16
NT = (((1,), (1,)), ((), ()))
TN = (((0,), (0,)), ((), ()))
CHUNKS = 4
DIRECT = 2
COPIES = 70
MAIN_VMEM = 50 * 2**20
GRAD_VMEM = 24 * 2**20


def dot(a, b, dims=(((1,), (0,)), ((), ()))):
    return lax.dot_general(a, b, dims, preferred_element_type=F32)


def slot_capacity(tokens_dev, top_k, n_experts):
    return 8 * ((3 * top_k * tokens_dev + 16 * n_experts - 1) // (16 * n_experts))


def scoped(name):
    def deco(fn):
        def run(*args, **kw):
            tag = "_".join([name] + [str(getattr(a, "tag", a)) for a in args if isinstance(a, (int, Gather))])
            with jax.named_scope(tag):
                return fn(*args, **kw)
        return run
    return deco


class Link:
    def __init__(self, send, recv):
        self.send, self.recv, self.used, self.pending = send, recv, 0, {}

    def copy(self, src, dst, device):
        k = self.used
        self.used += 1
        c = pltpu.make_async_remote_copy(
            src_ref=src, dst_ref=dst, send_sem=self.send.at[k], recv_sem=self.recv.at[k],
            device_id={"expert": device}, device_id_type=MESH)
        return k, c

    def start(self, kc):
        k, c = kc
        if k in self.pending:
            self.pending[k].wait_send()
        c.start()
        self.pending[k] = c

    @scoped("drain")
    def drain(self):
        for c in self.pending.values():
            c.wait_send()


class Gather:
    def __init__(self, link, place, own, buf, split, tag, direct=False):
        me, partner, left, right, far = place
        self.link, self.tag, self.direct = link, tag, direct
        half = own.shape[0] // 2
        a, b = pl.ds(0, half), pl.ds(half, half)
        self.pair = link.copy(own, buf.at[me], partner)
        if direct:
            self.first = [link.copy(own, buf.at[me], right), link.copy(own, buf.at[me], left)]
            self.second = []
            self.relay = [link.copy(own, buf.at[me], far)]
            far_pair = [link.copy(buf.at[far], buf.at[far], partner)]
        elif split:
            self.first = [link.copy(own.at[a], buf.at[me, a], right), link.copy(own.at[b], buf.at[me, b], left)]
            self.second = [link.copy(own.at[b], buf.at[me, b], right), link.copy(own.at[a], buf.at[me, a], left)]
            self.relay = [link.copy(buf.at[left, a], buf.at[left, a], right), link.copy(buf.at[right, b], buf.at[right, b], left)]
            far_pair = [link.copy(buf.at[far], buf.at[far], partner)]
        else:
            self.first = [link.copy(own, buf.at[me], right), link.copy(own, buf.at[me], left)]
            self.second = []
            self.relay = [link.copy(buf.at[left], buf.at[left], right)]
            far_pair = [link.copy(buf.at[far], buf.at[far], partner)]
        self.near_pair = [link.copy(buf.at[left], buf.at[left], partner), link.copy(buf.at[right], buf.at[right], partner)]
        self.far_pair = far_pair

    @scoped("ag_begin_first")
    def begin_first(self):
        for c in self.first:
            self.link.start(c)

    @scoped("ag_begin")
    def begin(self, first=True):
        for c in (self.relay if self.direct else []) + (self.first if first else []) + self.second + [self.pair]:
            self.link.start(c)

    @scoped("ag_forward")
    def forward(self):
        for c in self.first:
            c[1].wait_recv()
        for c in [] if self.direct else self.relay:
            self.link.start(c)

    @scoped("ag_share_near")
    def share_near(self):
        for c in self.second:
            c[1].wait_recv()
        for c in self.near_pair:
            self.link.start(c)

    @scoped("ag_share_far")
    def share_far(self):
        for c in self.relay:
            c[1].wait_recv()
        for c in self.far_pair:
            self.link.start(c)

    @scoped("ag_finish")
    def finish(self):
        for c in [self.pair] + self.near_pair + self.far_pair:
            c[1].wait_recv()


def main_kernel(dims, x_in, y_in, dy_in, e1_in, g1_in, s1_in, e2_in, g2_in, s2_in, wg1, wu1, wd1, wg2, wu2, wd2,
                saved, own_o, dmid_o, qr_o, ql_o, qf_o,
                tok, route, gate, wv, rt, rtg, yg, gg, xg, dg, oh, ot, grow, act_a, act_b, dhp, dxb,
                d1own, q, sd, rd, ra, rb, fl, fr, send, recv, isem, wsem):
    n_dev, tokens, model, ffn, n_local, cap = dims
    n_chips = n_dev // 2
    me = lax.axis_index("expert")
    chip, core = me // 2, lax.rem(me, 2)
    partner = chip * 2 + 1 - core
    right = lax.rem(chip + 1, n_chips) * 2 + core
    left = lax.rem(chip + n_chips - 1, n_chips) * 2 + core
    far = lax.rem(chip + 2, n_chips) * 2 + core
    place = (me, partner, left, right, far)
    rows_chip = 2 * cap
    rows = n_local * rows_chip
    cw = model // CHUNKS
    half = tokens // 2
    u, z, h, da, db = ([saved[i], saved[5 + i]] for i in range(5))

    barrier = pltpu.get_barrier_semaphore()
    for d in (partner, left, right, far):
        pl.semaphore_signal(barrier, inc=1, device_id={"expert": d}, device_id_type=MESH)

    x_ref, y_ref, dy_ref = tok
    hw = model // 2
    e1, s1, e2, s2 = route
    g1, g2 = gate
    loads = []
    for i, (r, v) in enumerate(((e1_in, e1), (g1_in, g1), (s1_in, s1), (e2_in, e2), (g2_in, g2), (s2_in, s2), (y_in, y_ref), (x_in, x_ref), (dy_in.at[:, 0:hw], dy_ref.at[0]), (dy_in.at[:, hw:], dy_ref.at[1]))):
        c = pltpu.make_async_copy(r, v, isem.at[i])
        c.start()
        loads.append(c)
    for c in loads[:7]:
        c.wait()

    w_a, w_b, w_c, w_d, w_e, w_f = wv
    wload = {}

    def load(name, src, dst):
        wload[name] = pltpu.make_async_copy(src, dst, wsem.at[len(wload)])
        wload[name].start()

    def need(*names):
        with jax.named_scope("wload"):
            for name in names:
                wload.pop(name).wait()
                wload[name + " done"] = None

    load("down2", wd2, w_c)
    load("gate2", wg2, w_a)
    load("up2", wu2, w_b)
    load("down1", wd1, w_f)

    def target(experts, slots):
        return jnp.where(slots >= 0, experts * rows_chip + core * cap + slots, -1).astype(F32)

    top_k = e1.shape[0]
    rt[0:top_k, 0:tokens] = target(e2[...], s2[...])
    rt[0:top_k, tokens:2 * tokens] = target(e1[...], s1[...])
    rt[top_k:2 * top_k, 0:tokens] = g2[...]
    rt[top_k:2 * top_k, tokens:2 * tokens] = g1[...]

    link = Link(send, recv)
    g_rt = Gather(link, place, rt, rtg, False, "rt", direct=True)
    g_y = Gather(link, place, y_ref, yg, True, "y")
    g_g = [Gather(link, place, dy_ref.at[i], gg.at[i], True, f"g{i}") for i in range(2)]
    g_x = Gather(link, place, x_ref, xg, True, "x")
    rtg[me] = rt[...]
    yg[me] = y_ref[...]
    for c in loads[7:]:
        c.wait()
    for i in range(2):
        gg[i, me] = dy_ref[i]
    xg[me] = x_ref[...]

    with jax.named_scope("barrier"):
        pl.semaphore_wait(barrier, 4)

    @scoped("build")
    def build(layer):
        lane = lax.broadcasted_iota(jnp.int32, (top_k, 2 * tokens), 1)
        rid = lax.broadcasted_iota(jnp.int32, (rows, 2 * tokens), 0).astype(F32)
        base = (me * (n_local * rows_chip)).astype(F32)

        def one(c, carry):
            r0, r1 = rtg[2 * c], rtg[2 * c + 1]

            def pick(lo):
                p0, p1 = r0[lo:lo + top_k], r1[lo:lo + top_k]
                if layer == 0:
                    return jnp.where(lane < tokens, p0, pltpu.roll(p1, tokens, 1))
                return jnp.where(lane < tokens, pltpu.roll(p0, tokens, 1), p1)

            t, g = pick(0) - base, pick(top_k)
            hit = jnp.zeros((rows, 2 * tokens), F32)
            gm = jnp.zeros((rows, 2 * tokens), F32)
            for j in range(top_k):
                m = t[j:j + 1] == rid
                hit = jnp.where(m, 1.0, hit)
                gm = jnp.where(m, g[j:j + 1], gm)
            oh[layer, c] = hit.astype(BF16)
            ot[layer, c] = hit.T.astype(BF16)
            grow[layer, c] = jnp.sum(gm, axis=1, keepdims=True)
            return carry

        lax.fori_loop(0, n_chips, one, 0)

    @scoped("rows_of")
    def rows_of(layer, buf, dst, gated, cols=None):
        lo, width = (0, model) if cols is None else cols
        for c in range(n_chips):
            src = jnp.concatenate([buf[2 * c], buf[2 * c + 1]], axis=0)
            r = dot(oh[layer, c], src)
            if gated:
                r = r * grow[layer, c]
            r = r.astype(BF16)
            for e in range(n_local):
                dst[e, c * rows_chip:(c + 1) * rows_chip, lo:lo + width] = r[e * rows_chip:(e + 1) * rows_chip]

    @scoped("forward_act")
    def forward_act(layer, e):
        ue = u[layer][e]
        aw = dot(ue, w_a[e]).astype(BF16).astype(F32)
        bw = dot(ue, w_b[e]).astype(BF16).astype(F32)
        sig = jax.nn.sigmoid(aw)
        silu = aw * sig
        h[layer][e] = (silu * bw).astype(BF16)
        act_a[e] = bw * sig * (1.0 + aw * (1.0 - sig))
        act_b[e] = silu

    @scoped("back_part")
    def back_part(layer, width):
        for e in range(n_local):
            dhp[e] = dot(z[layer][e, :, :width], w_d[e, :width])

    @scoped("back_act")
    def back_act(layer, lo):
        for e in range(n_local):
            dh = dot(z[layer][e, :, lo:], w_d[e, lo:])
            if lo:
                dh = dh + dhp[e]
            da[layer][e] = (dh * act_a[e]).astype(BF16)
            db[layer][e] = (dh * act_b[e]).astype(BF16)

    @scoped("flip")
    def flip(src, dst, lo=0, hi=n_local):
        def body(e, carry):
            dst[e] = src[e].T
            return carry
        lax.fori_loop(lo, hi, body, 0)

    gate_t, up_t = (w_c, w_f), (w_e, w_c)

    @scoped("dx_chunk")
    def dx_chunk(layer, k):
        cols = slice(k * cw, (k + 1) * cw)
        for e in range(n_local):
            d = dot(da[layer][e], gate_t[layer][e, :, cols]) + dot(db[layer][e], up_t[layer][e, :, cols])
            d = d.astype(BF16)
            for c in range(n_chips):
                dxb[k, c, e * rows_chip:(e + 1) * rows_chip] = d[c * rows_chip:(c + 1) * rows_chip]
        for c in range(n_chips):
            q[layer, k, c] = dot(ot[layer, c], dxb[k, c])

    mine, theirs = pl.multiple_of(core * tokens, tokens), pl.multiple_of((1 - core) * tokens, tokens)

    pair, base = {}, link.used
    for layer in range(2):
        link.used = base
        for k in range(CHUNKS):
            pair[layer, k] = link.copy(q.at[layer, k, :, pl.ds(theirs, tokens)], rd.at[layer, k], partner)
    rs_far = [[link.copy(sd.at[k, far // 2, pl.ds(0, half)], ra.at[k], right),
               link.copy(sd.at[k, far // 2, pl.ds(half, half)], rb.at[k], left)] for k in range(CHUNKS)]
    rs_near = [[link.copy(sd.at[k, right // 2], fl.at[k], right),
                link.copy(sd.at[k, left // 2], fr.at[k], left)] for k in range(CHUNKS)]
    link.used = 0
    ag = [Gather(link, place, d1own.at[k], dg.at[k], True, k, direct=k >= CHUNKS - DIRECT) for k in range(CHUNKS)]

    @scoped("stage_far")
    def stage_far(k):
        pair[0, k][1].wait_recv()
        sd[k] = q[0, k, :, pl.ds(mine, tokens)] + rd[0, k]
        for c in rs_far[k]:
            link.start(c)

    @scoped("stage_near")
    def stage_near(k):
        for c in rs_far[k]:
            c[1].wait_recv()
        sd[k, right // 2, 0:half] = sd[k, right // 2, 0:half] + ra[k]
        sd[k, left // 2, half:] = sd[k, left // 2, half:] + rb[k]
        for c in rs_near[k]:
            link.start(c)

    @scoped("stage_sum")
    def stage_sum(k):
        for c in rs_near[k]:
            c[1].wait_recv()
        total = sd[k, chip] + (fl[k] + fr[k])
        d = (dy_ref[k * cw // hw, :, k * cw % hw:k * cw % hw + cw].astype(F32) + total).astype(BF16)
        d1own[k] = d
        dg[k, me] = d
        dmid_o[:, k * cw:(k + 1) * cw] = d
        ag[k].begin()

    @scoped("stage_out")
    def stage_out(k):
        pair[1, k][1].wait_recv()
        cols = slice(k * cw, (k + 1) * cw)
        for c, o in ((chip, own_o), (right // 2, qr_o), (left // 2, ql_o), (far // 2, qf_o)):
            o[:, cols] = q[1, k, c, pl.ds(mine, tokens)] + rd[1, k, c]

    def z_chunk(k):
        ag[k].finish()
        rows_of(1, dg.at[k], z[1], True, (k * cw, cw))

    g_rt.begin()
    g_y.begin()
    g_g[0].begin()
    need("down2")
    flip(w_c, w_d)
    g_rt.forward()
    g_rt.share_near()
    g_y.forward()
    g_g[1].begin()
    g_rt.share_far()
    g_y.share_near()
    g_rt.finish()
    build(0)
    need("gate2")
    flip(w_a, w_c)
    g_y.share_far()
    g_g[0].forward()
    g_g[1].forward()
    g_x.begin()
    need("up2")
    flip(w_b, w_e)
    g_y.finish()
    rows_of(0, yg, u[0], False)
    g_g[0].share_near()
    g_g[1].share_near()
    forward_act(0, 0)
    g_g[0].share_far()
    forward_act(0, 1)
    forward_act(0, 2)
    g_g[1].share_far()
    forward_act(0, 3)
    load("gate1", wg1, w_a)
    load("up1", wu1, w_b)
    g_g[0].finish()
    rows_of(0, gg.at[0], z[0], True, (0, hw))
    g_g[1].finish()
    rows_of(0, gg.at[1], z[0], True, (hw, hw))
    back_act(0, 0)
    g_x.forward()

    for k in range(CHUNKS):
        dx_chunk(0, k)
        link.start(pair[0, k])
        if k == 0:
            g_x.share_near()
        if k >= 1:
            stage_far(k - 1)
    need("down1")
    flip(w_f, w_d, 0, 2)
    stage_far(CHUNKS - 1)
    g_x.share_far()
    flip(w_f, w_d, 2, 4)
    stage_near(0)
    build(1)
    stage_near(1)
    g_x.finish()
    rows_of(1, xg, u[1], False)
    stage_near(2)
    need("gate1", "up1")
    forward_act(1, 0)
    stage_near(3)
    flip(w_b, w_c, 0, 2)
    stage_sum(0)
    forward_act(1, 1)
    stage_sum(1)
    forward_act(1, 2)
    stage_sum(2)
    flip(w_b, w_c, 2, 4)
    ag[0].forward()
    stage_sum(3)
    ag[1].forward()
    ag[0].share_near()
    ag[1].share_near()
    ag[2].forward()
    forward_act(1, 3)
    flip(w_a, w_f, 0, 2)
    ag[0].share_far()
    ag[3].forward()
    ag[2].share_near()
    ag[1].share_far()
    ag[3].share_near()
    ag[2].share_far()
    flip(w_a, w_f, 2, 4)
    z_chunk(0)
    z_chunk(1)
    ag[3].share_far()
    back_part(1, hw)
    z_chunk(2)
    z_chunk(3)

    back_act(1, hw)
    for k in range(CHUNKS):
        dx_chunk(1, k)
        link.start(pair[1, k])
        if k >= 2:
            stage_out(k - 2)
    stage_out(CHUNKS - 2)
    stage_out(CHUNKS - 1)

    link.drain()


def grad_kernel(n_local, *refs):
    ins, outs = refs[:10], refs[10:16]
    vout, osem = refs[16:]

    def store(i, layer, e, s):
        return pltpu.make_async_copy(vout[i].at[s], outs[3 * layer + i].at[e], osem.at[i, s])

    for layer in range(2):
        u, z, h, da, db = ins[5 * layer:5 * layer + 5]

        def body(e, carry, layer=layer, u=u, z=z, h=h, da=da, db=db):
            s = lax.rem(e, 2)
            for i, (a, b) in enumerate(((u, da), (u, db), (h, z))):
                def reclaim(i=i):
                    store(i, layer, e, s).wait()

                if layer == 0:
                    pl.when(e >= 2)(reclaim)
                else:
                    reclaim()
                vout[i][s] = dot(a[e], b[e], TN)
                store(i, layer, e, s).start()
            return carry

        lax.fori_loop(0, n_local, body, 0)
    for s in range(2):
        for i in range(3):
            store(i, 1, n_local - 2 + s, s).wait()


def solution(mesh):
    n_dev = mesh.shape["expert"]
    tok_spec = P(("data", "expert"), None)
    weight_spec = P("expert", None, None)
    grad_spec = P(("data", "expert"), None, None)

    def local_step(x, y, dy, experts_one, gates_one, slots_one, experts_two, gates_two, slots_two, wg1, wu1, wd1, wg2, wu2, wd2):
        tokens, model = x.shape
        n_local, _, ffn = wg1.shape
        top_k = experts_one.shape[1]
        cap = slot_capacity(tokens, top_k, n_local * n_dev)
        n_chips = n_dev // 2
        rows = n_local * 2 * cap
        cw = model // CHUNKS
        half = tokens // 2

        S = jax.ShapeDtypeStruct
        er = n_chips * 2 * cap
        wide, narrow = S((n_local, er, model), BF16), S((n_local, er, ffn), BF16)
        saved = [wide, wide, narrow, narrow, narrow]
        part = S((tokens, model), F32)
        hbm, vm = pl.BlockSpec(memory_space=pltpu.HBM), pl.BlockSpec(memory_space=pltpu.VMEM)
        V = pltpu.VMEM
        scratch = [
            [V((tokens, model), BF16), V((tokens, model), BF16), V((2, tokens, model // 2), BF16)], [V((top_k, tokens), jnp.int32)] * 4, [V((top_k, tokens), F32)] * 2,
            [V(w.shape, BF16) for w in (wg2, wg2, wd2, wg2, wd2, wd2)],
            V((2 * top_k, 2 * tokens), F32), V((n_dev, 2 * top_k, 2 * tokens), F32),
            V((n_dev, tokens, model), BF16), V((2, n_dev, tokens, model // 2), BF16), V((n_dev, tokens, model), BF16),
            V((CHUNKS, n_dev, tokens, cw), BF16),
            V((2, n_chips, rows, 2 * tokens), BF16), V((2, n_chips, 2 * tokens, rows), BF16), V((2, n_chips, rows, 1), F32),
            V((n_local, er, ffn), F32), V((n_local, er, ffn), F32), V((n_local, er, ffn), F32),
            V((CHUNKS, n_chips, rows, cw), BF16),
            V((CHUNKS, tokens, cw), BF16),
            V((2, CHUNKS, n_chips, 2 * tokens, cw), F32),
            V((CHUNKS, n_chips, tokens, cw), F32),
            V((2, CHUNKS, n_chips, tokens, cw), F32),
            V((CHUNKS, half, cw), F32), V((CHUNKS, half, cw), F32),
            V((CHUNKS, tokens, cw), F32), V((CHUNKS, tokens, cw), F32),
            pltpu.SemaphoreType.DMA((COPIES,)), pltpu.SemaphoreType.DMA((COPIES,)),
            pltpu.SemaphoreType.DMA((10,)), pltpu.SemaphoreType.DMA((6,)),
        ]
        kept, own, dmid, q_right, q_left, q_far = pl.pallas_call(
            functools.partial(main_kernel, (n_dev, tokens, model, ffn, n_local, cap)),
            out_shape=[[V(s.shape, s.dtype) for s in saved + saved], V(part.shape, F32), V(part.shape, BF16)] + [V(part.shape, F32)] * 3,
            in_specs=[hbm] * 15,
            out_specs=[[vm] * 10, vm, vm, vm, vm, vm],
            scratch_shapes=scratch,
            compiler_params=pltpu.CompilerParams(collective_id=0, has_side_effects=True, vmem_limit_bytes=MAIN_VMEM),
            name="moe_main",
        )(x, y, dy, experts_one.T, gates_one.T, slots_one.T, experts_two.T, gates_two.T, slots_two.T, wg1, wu1, wd1, wg2, wu2, wd2)

        def shift(v, by):
            return lax.ppermute(v, "expert", [(i, (i + by) % n_dev) for i in range(n_dev)])

        from_left, from_right, from_far = shift(q_right, 2), shift(q_left, n_dev - 2), shift(q_far, n_dev // 2)

        up, down = S((n_local, model, ffn), F32), S((n_local, ffn, model), F32)
        flops = 2 * 2 * n_local * er * model * ffn * 3
        grads = pl.pallas_call(
            functools.partial(grad_kernel, n_local),
            out_shape=[up, up, down] * 2,
            in_specs=[vm] * 10,
            out_specs=[hbm] * 6,
            scratch_shapes=[
                [V((2, model, ffn), F32), V((2, model, ffn), F32), V((2, ffn, model), F32)],
                pltpu.SemaphoreType.DMA((3, 2))],
            compiler_params=pltpu.CompilerParams(vmem_limit_bytes=GRAD_VMEM),
            cost_estimate=pl.CostEstimate(flops=flops, bytes_accessed=6 * n_local * model * ffn * 4, transcendentals=0),
            name="moe_grads",
        )(*kept)
        dx = (dmid.astype(F32) + ((own + from_far) + (from_left + from_right))).astype(BF16)
        return (dx,) + tuple(grads[3:]) + tuple(grads[:3])

    return jax.shard_map(local_step, mesh=mesh, in_specs=(tok_spec,) * 9 + (weight_spec,) * 6, out_specs=(tok_spec,) + (grad_spec,) * 6, check_vma=False)
```

```python
import functools
import jax
import jax.numpy as jnp
from jax import lax
from jax.experimental import pallas as pl
from jax.experimental.pallas import tpu as pltpu
from jax.sharding import PartitionSpec as P

MESH = pl.DeviceIdType.MESH
F32 = jnp.float32
BF16 = jnp.bfloat16
NT = (((1,), (1,)), ((), ()))
TN = (((0,), (0,)), ((), ()))
CHUNKS = 4
DIRECT = 1
COPIES = 67
MAIN_VMEM = 50 * 2**20
GRAD_VMEM = 24 * 2**20


def dot(a, b, dims=(((1,), (0,)), ((), ()))):
    return lax.dot_general(a, b, dims, preferred_element_type=F32)


def slot_capacity(tokens_dev, top_k, n_experts):
    return 8 * ((3 * top_k * tokens_dev + 16 * n_experts - 1) // (16 * n_experts))


def scoped(name):
    def deco(fn):
        def run(*args, **kw):
            tag = "_".join([name] + [str(getattr(a, "tag", a)) for a in args if isinstance(a, (int, Gather))])
            with jax.named_scope(tag):
                return fn(*args, **kw)
        return run
    return deco


class Link:
    def __init__(self, send, recv):
        self.send, self.recv, self.used, self.sets, self.sent = send, recv, 0, -1, []

    def new_set(self, sent):
        self.sets += 1
        self.sent.append(sent)

    def copy(self, src, dst, device):
        k = self.used
        self.used += 1
        return pltpu.make_async_remote_copy(
            src_ref=src, dst_ref=dst, send_sem=self.send.at[self.sets], recv_sem=self.recv.at[k],
            device_id={"expert": device}, device_id_type=MESH)

    def start(self, c):
        c.start()

    @scoped("drain")
    def drain(self, device):
        for i, ref in enumerate(self.sent):
            pltpu.make_async_remote_copy(
                src_ref=ref, dst_ref=ref, send_sem=self.send.at[i], recv_sem=self.recv.at[0],
                device_id={"expert": device}, device_id_type=MESH).wait_send()


class Gather:
    def __init__(self, link, place, own, buf, split, tag, direct=False):
        me, partner, left, right, far = place
        self.link, self.tag, self.direct = link, tag, direct
        link.new_set(buf.at[pl.ds(0, 7)])
        half = own.shape[0] // 2
        a, b = pl.ds(0, half), pl.ds(half, half)
        self.pair = link.copy(own, buf.at[me], partner)
        if direct:
            self.first = [link.copy(own, buf.at[me], right), link.copy(own, buf.at[me], left)]
            self.second = []
            self.relay = [link.copy(own, buf.at[me], far)]
            far_pair = [link.copy(buf.at[far], buf.at[far], partner)]
        elif split:
            self.first = [link.copy(own.at[a], buf.at[me, a], right), link.copy(own.at[b], buf.at[me, b], left)]
            self.second = [link.copy(own.at[b], buf.at[me, b], right), link.copy(own.at[a], buf.at[me, a], left)]
            self.relay = [link.copy(buf.at[left, a], buf.at[left, a], right), link.copy(buf.at[right, b], buf.at[right, b], left)]
            far_pair = [link.copy(buf.at[far], buf.at[far], partner)]
        else:
            self.first = [link.copy(own, buf.at[me], right), link.copy(own, buf.at[me], left)]
            self.second = []
            self.relay = [link.copy(buf.at[left], buf.at[left], right)]
            far_pair = [link.copy(buf.at[far], buf.at[far], partner)]
        self.near_pair = [link.copy(buf.at[left], buf.at[left], partner), link.copy(buf.at[right], buf.at[right], partner)]
        self.far_pair = far_pair

    @scoped("ag_begin")
    def begin(self):
        for c in (self.relay if self.direct else []) + self.first + self.second + [self.pair]:
            self.link.start(c)

    @scoped("ag_forward")
    def forward(self):
        for c in self.first:
            c.wait_recv()
        for c in [] if self.direct else self.relay:
            self.link.start(c)

    @scoped("ag_share_near")
    def share_near(self):
        for c in self.second:
            c.wait_recv()
        for c in self.near_pair:
            self.link.start(c)

    @scoped("ag_share_far")
    def share_far(self):
        for c in self.relay:
            c.wait_recv()
        for c in self.far_pair:
            self.link.start(c)

    @scoped("ag_finish")
    def finish(self):
        for c in [self.pair] + self.near_pair + self.far_pair:
            c.wait_recv()


def main_kernel(dims, x_in, y_in, dy_in, e1_in, g1_in, s1_in, e2_in, g2_in, s2_in, wg1, wu1, wd1, wg2, wu2, wd2,
                saved, own_o, dmid_o, qr_o, ql_o, qf_o,
                tok, route, gate, wv, rt, rtg, yg, gg, xg, dg, oh, ot, grow, act_a, act_b, dhp, dxb,
                d1own, q, sd, rd, ra, rb, fl, fr, send, recv, isem, wsem):
    n_dev, tokens, model, ffn, n_local, cap = dims
    n_chips = n_dev // 2
    me = lax.axis_index("expert")
    chip, core = me // 2, lax.rem(me, 2)
    partner = chip * 2 + 1 - core
    right = lax.rem(chip + 1, n_chips) * 2 + core
    left = lax.rem(chip + n_chips - 1, n_chips) * 2 + core
    far = lax.rem(chip + 2, n_chips) * 2 + core
    place = (me, partner, left, right, far)
    rows_chip = 2 * cap
    rows = n_local * rows_chip
    cw = model // CHUNKS
    half = tokens // 2
    u, z, h, da, db = ([saved[i], saved[5 + i]] for i in range(5))

    barrier = pltpu.get_barrier_semaphore()
    for d in (partner, left, right, far):
        pl.semaphore_signal(barrier, inc=1, device_id={"expert": d}, device_id_type=MESH)

    x_ref, y_ref, dy_ref = tok
    hw = model // 2
    e1, s1, e2, s2 = route
    g1, g2 = gate
    loads = []
    for i, (r, v) in enumerate(((e1_in, e1), (g1_in, g1), (s1_in, s1), (e2_in, e2), (g2_in, g2), (s2_in, s2), (y_in, y_ref), (x_in, x_ref), (dy_in.at[:, 0:hw], dy_ref.at[0]), (dy_in.at[:, hw:], dy_ref.at[1]))):
        c = pltpu.make_async_copy(r, v, isem.at[i])
        c.start()
        loads.append(c)
    for c in loads[:7]:
        c.wait()

    w_a, w_b, w_c, w_d, w_e, w_f = wv
    wload = {}

    def load(name, src, dst):
        wload[name] = pltpu.make_async_copy(src, dst, wsem.at[len(wload)])
        wload[name].start()

    def need(*names):
        with jax.named_scope("wload"):
            for name in names:
                wload.pop(name).wait()
                wload[name + " done"] = None

    load("down2", wd2, w_c)
    load("gate2", wg2, w_a)
    load("up2", wu2, w_b)
    load("down1", wd1, w_f)

    def target(experts, slots):
        return jnp.where(slots >= 0, experts * rows_chip + core * cap + slots, -1).astype(F32)

    top_k = e1.shape[0]
    rt[0:top_k, 0:tokens] = target(e2[...], s2[...])
    rt[0:top_k, tokens:2 * tokens] = target(e1[...], s1[...])
    rt[top_k:2 * top_k, 0:tokens] = g2[...]
    rt[top_k:2 * top_k, tokens:2 * tokens] = g1[...]

    link = Link(send, recv)
    g_rt = Gather(link, place, rt, rtg, False, "rt", direct=True)
    g_y = Gather(link, place, y_ref, yg, True, "y")
    g_g = [Gather(link, place, dy_ref.at[i], gg.at[i], True, f"g{i}") for i in range(2)]
    g_x = Gather(link, place, x_ref, xg, True, "x")
    with jax.named_scope("barrier"):
        pl.semaphore_wait(barrier, 4)

    @scoped("build")
    def build(layer):
        lane = lax.broadcasted_iota(jnp.int32, (top_k, 2 * tokens), 1)
        rid = lax.broadcasted_iota(jnp.int32, (rows, 2 * tokens), 0).astype(F32)
        base = (me * (n_local * rows_chip)).astype(F32)

        def one(c, carry):
            r0, r1 = rtg[2 * c], rtg[2 * c + 1]

            def pick(lo):
                p0, p1 = r0[lo:lo + top_k], r1[lo:lo + top_k]
                if layer == 0:
                    return jnp.where(lane < tokens, p0, pltpu.roll(p1, tokens, 1))
                return jnp.where(lane < tokens, pltpu.roll(p0, tokens, 1), p1)

            t, g = pick(0) - base, pick(top_k)
            hit = jnp.zeros((rows, 2 * tokens), F32)
            gm = jnp.zeros((rows, 2 * tokens), F32)
            for j in range(top_k):
                m = t[j:j + 1] == rid
                hit = jnp.where(m, 1.0, hit)
                gm = jnp.where(m, g[j:j + 1], gm)
            oh[layer, c] = hit.astype(BF16)
            ot[layer, c] = hit.T.astype(BF16)
            grow[layer, c] = jnp.sum(gm, axis=1, keepdims=True)
            return carry

        lax.fori_loop(0, n_chips, one, 0)

    @scoped("rows_of")
    def rows_of(layer, buf, dst, gated, cols=None):
        lo, width = (0, model) if cols is None else cols
        for c in range(n_chips):
            src = jnp.concatenate([buf[2 * c], buf[2 * c + 1]], axis=0)
            r = dot(oh[layer, c], src)
            if gated:
                r = r * grow[layer, c]
            r = r.astype(BF16)
            for e in range(n_local):
                dst[e, c * rows_chip:(c + 1) * rows_chip, lo:lo + width] = r[e * rows_chip:(e + 1) * rows_chip]

    @scoped("forward_act")
    def forward_act(layer, e):
        ue = u[layer][e]
        aw = dot(ue, w_a[e]).astype(BF16).astype(F32)
        bw = dot(ue, w_b[e]).astype(BF16).astype(F32)
        sig = jax.nn.sigmoid(aw)
        silu = aw * sig
        h[layer][e] = (silu * bw).astype(BF16)
        act_a[e] = bw * sig * (1.0 + aw * (1.0 - sig))
        act_b[e] = silu

    @scoped("back_part")
    def back_part(layer, width):
        for e in range(n_local):
            dhp[e] = dot(z[layer][e, :, :width], w_d[e, :width])

    @scoped("back_act")
    def back_act(layer, lo):
        for e in range(n_local):
            dh = dot(z[layer][e, :, lo:], w_d[e, lo:])
            if lo:
                dh = dh + dhp[e]
            da[layer][e] = (dh * act_a[e]).astype(BF16)
            db[layer][e] = (dh * act_b[e]).astype(BF16)

    @scoped("flip")
    def flip(src, dst, lo=0, hi=n_local):
        def body(e, carry):
            dst[e] = src[e].T
            return carry
        lax.fori_loop(lo, hi, body, 0)

    gate_t, up_t = (w_c, w_f), (w_e, w_c)

    @scoped("dx_chunk")
    def dx_chunk(layer, k):
        cols = slice(k * cw, (k + 1) * cw)
        for e in range(n_local):
            d = dot(da[layer][e], gate_t[layer][e, :, cols]) + dot(db[layer][e], up_t[layer][e, :, cols])
            d = d.astype(BF16)
            for c in range(n_chips):
                dxb[k, c, e * rows_chip:(e + 1) * rows_chip] = d[c * rows_chip:(c + 1) * rows_chip]
        for c in range(n_chips):
            q[layer, k, c] = dot(ot[layer, c], dxb[k, c])

    mine, theirs = pl.multiple_of(core * tokens, tokens), pl.multiple_of((1 - core) * tokens, tokens)

    pair, rs_far, rs_near, base = {}, [], [], link.used
    for k in range(CHUNKS):
        link.new_set(q.at[0, k, :, pl.ds(0, 7 * tokens // n_chips)])
        pair[0, k] = link.copy(q.at[0, k, :, pl.ds(theirs, tokens)], rd.at[0, k], partner)
        rs_far.append([link.copy(sd.at[k, far // 2, pl.ds(0, half)], ra.at[k], right),
                       link.copy(sd.at[k, far // 2, pl.ds(half, half)], rb.at[k], left)])
        rs_near.append([link.copy(sd.at[k, right // 2], fl.at[k], right),
                        link.copy(sd.at[k, left // 2], fr.at[k], left)])
    end = link.used
    link.new_set(rd.at[1])
    for k in range(CHUNKS):
        link.used = base + 5 * k
        pair[1, k] = link.copy(q.at[1, k, :, pl.ds(theirs, tokens)], rd.at[1, k], partner)
    link.used = end
    link.used = 0
    ag = [Gather(link, place, d1own.at[k], dg.at[k], True, k, direct=k >= CHUNKS - DIRECT) for k in range(CHUNKS)]

    @scoped("stage_far")
    def stage_far(k):
        pair[0, k].wait_recv()
        sd[k] = q[0, k, :, pl.ds(mine, tokens)] + rd[0, k]
        for c in rs_far[k]:
            link.start(c)

    @scoped("stage_near")
    def stage_near(k):
        for c in rs_far[k]:
            c.wait_recv()
        sd[k, right // 2, 0:half] = sd[k, right // 2, 0:half] + ra[k]
        sd[k, left // 2, half:] = sd[k, left // 2, half:] + rb[k]
        for c in rs_near[k]:
            link.start(c)

    @scoped("stage_sum")
    def stage_sum(k):
        for c in rs_near[k]:
            c.wait_recv()
        total = sd[k, chip] + (fl[k] + fr[k])
        d = (dy_ref[k * cw // hw, :, k * cw % hw:k * cw % hw + cw].astype(F32) + total).astype(BF16)
        d1own[k] = d
        dg[k, me] = d
        dmid_o[:, k * cw:(k + 1) * cw] = d
        ag[k].begin()

    @scoped("stage_out")
    def stage_out(k):
        pair[1, k].wait_recv()
        cols = slice(k * cw, (k + 1) * cw)
        for c, o in ((chip, own_o), (right // 2, qr_o), (left // 2, ql_o), (far // 2, qf_o)):
            o[:, cols] = q[1, k, c, pl.ds(mine, tokens)] + rd[1, k, c]

    def z_chunk(k):
        ag[k].finish()
        rows_of(1, dg.at[k], z[1], True, (k * cw, cw))

    g_rt.begin()
    g_y.begin()
    for c in loads[7:]:
        c.wait()
    g_g[0].begin()
    rtg[me] = rt[...]
    yg[me] = y_ref[...]
    xg[me] = x_ref[...]
    for i in range(2):
        gg[i, me] = dy_ref[i]
    need("down2")
    flip(w_c, w_d)
    g_rt.forward()
    g_rt.share_near()
    g_y.forward()
    g_g[1].begin()
    g_rt.share_far()
    need("gate2")
    flip(w_a, w_c)
    g_y.share_near()
    g_rt.finish()
    build(0)
    g_g[0].forward()
    need("up2")
    flip(w_b, w_e, 0, 3)
    g_y.share_far()
    g_g[1].forward()
    g_x.begin()
    flip(w_b, w_e, 3, 4)
    g_g[0].share_near()
    g_y.finish()
    rows_of(0, yg, u[0], False)
    forward_act(0, 0)
    g_g[1].share_near()
    forward_act(0, 1)
    g_g[0].share_far()
    forward_act(0, 2)
    g_g[1].share_far()
    forward_act(0, 3)
    load("gate1", wg1, w_a)
    load("up1", wu1, w_b)
    g_g[0].finish()
    rows_of(0, gg.at[0], z[0], True, (0, hw))
    g_g[1].finish()
    rows_of(0, gg.at[1], z[0], True, (hw, hw))
    back_act(0, 0)
    g_x.forward()

    for k in range(CHUNKS):
        dx_chunk(0, k)
        link.start(pair[0, k])
        if k == 0:
            g_x.share_near()
        if k >= 1:
            stage_far(k - 1)
    need("down1")
    flip(w_f, w_d, 0, 2)
    stage_far(CHUNKS - 1)
    g_x.share_far()
    flip(w_f, w_d, 2, 4)
    stage_near(0)
    g_x.finish()
    build(1)
    stage_near(1)
    rows_of(1, xg, u[1], False)
    stage_near(2)
    need("gate1", "up1")
    forward_act(1, 0)
    stage_near(3)
    flip(w_b, w_c, 0, 4)
    stage_sum(0)
    forward_act(1, 1)
    forward_act(1, 2)
    stage_sum(1)
    forward_act(1, 3)
    flip(w_a, w_f, 0, 2)
    stage_sum(2)
    flip(w_a, w_f, 2, 4)
    stage_sum(3)
    ag[0].forward()
    ag[1].forward()
    ag[0].share_near()
    ag[1].share_near()
    ag[2].forward()
    ag[2].share_near()
    ag[0].share_far()
    ag[3].forward()
    ag[3].share_near()
    ag[1].share_far()
    ag[2].share_far()
    ag[3].share_far()
    z_chunk(0)
    z_chunk(1)
    back_part(1, hw)
    z_chunk(2)
    z_chunk(3)

    back_act(1, hw)
    for k in range(CHUNKS):
        dx_chunk(1, k)
        link.start(pair[1, k])
        if k >= 2:
            stage_out(k - 2)
    stage_out(CHUNKS - 2)
    stage_out(CHUNKS - 1)

    link.drain(partner)


def grad_kernel(n_local, *refs):
    ins, outs = refs[:10], refs[10:16]
    vout, osem = refs[16:]

    def store(i, layer, e, s):
        return pltpu.make_async_copy(vout[i].at[s], outs[3 * layer + i].at[e], osem.at[i, s])

    for layer in range(2):
        u, z, h, da, db = ins[5 * layer:5 * layer + 5]

        def body(e, carry, layer=layer, u=u, z=z, h=h, da=da, db=db):
            s = lax.rem(e, 2)
            for i, (a, b) in enumerate(((u, da), (u, db), (h, z))):
                def reclaim(i=i):
                    store(i, layer, e, s).wait()

                if layer == 0:
                    pl.when(e >= 2)(reclaim)
                else:
                    reclaim()
                vout[i][s] = dot(a[e], b[e], TN)
                store(i, layer, e, s).start()
            return carry

        lax.fori_loop(0, n_local, body, 0)
    for s in range(2):
        for i in range(3):
            store(i, 1, n_local - 2 + s, s).wait()


def solution(mesh):
    n_dev = mesh.shape["expert"]
    tok_spec = P(("data", "expert"), None)
    weight_spec = P("expert", None, None)
    grad_spec = P(("data", "expert"), None, None)

    def local_step(x, y, dy, experts_one, gates_one, slots_one, experts_two, gates_two, slots_two, wg1, wu1, wd1, wg2, wu2, wd2):
        tokens, model = x.shape
        n_local, _, ffn = wg1.shape
        top_k = experts_one.shape[1]
        cap = slot_capacity(tokens, top_k, n_local * n_dev)
        n_chips = n_dev // 2
        rows = n_local * 2 * cap
        cw = model // CHUNKS
        half = tokens // 2

        S = jax.ShapeDtypeStruct
        er = n_chips * 2 * cap
        wide, narrow = S((n_local, er, model), BF16), S((n_local, er, ffn), BF16)
        saved = [wide, wide, narrow, narrow, narrow]
        part = S((tokens, model), F32)
        hbm, vm = pl.BlockSpec(memory_space=pltpu.HBM), pl.BlockSpec(memory_space=pltpu.VMEM)
        V = pltpu.VMEM
        scratch = [
            [V((tokens, model), BF16), V((tokens, model), BF16), V((2, tokens, model // 2), BF16)], [V((top_k, tokens), jnp.int32)] * 4, [V((top_k, tokens), F32)] * 2,
            [V(w.shape, BF16) for w in (wg2, wg2, wd2, wg2, wd2, wd2)],
            V((2 * top_k, 2 * tokens), F32), V((n_dev, 2 * top_k, 2 * tokens), F32),
            V((n_dev, tokens, model), BF16), V((2, n_dev, tokens, model // 2), BF16), V((n_dev, tokens, model), BF16),
            V((CHUNKS, n_dev, tokens, cw), BF16),
            V((2, n_chips, rows, 2 * tokens), BF16), V((2, n_chips, 2 * tokens, rows), BF16), V((2, n_chips, rows, 1), F32),
            V((n_local, er, ffn), F32), V((n_local, er, ffn), F32), V((n_local, er, ffn), F32),
            V((CHUNKS, n_chips, rows, cw), BF16),
            V((CHUNKS, tokens, cw), BF16),
            V((2, CHUNKS, n_chips, 2 * tokens, cw), F32),
            V((CHUNKS, n_chips, tokens, cw), F32),
            V((2, CHUNKS, n_chips, tokens, cw), F32),
            V((CHUNKS, half, cw), F32), V((CHUNKS, half, cw), F32),
            V((CHUNKS, tokens, cw), F32), V((CHUNKS, tokens, cw), F32),
            pltpu.SemaphoreType.DMA((10 + CHUNKS,)), pltpu.SemaphoreType.DMA((COPIES,)),
            pltpu.SemaphoreType.DMA((10,)), pltpu.SemaphoreType.DMA((6,)),
        ]
        kept, own, dmid, q_right, q_left, q_far = pl.pallas_call(
            functools.partial(main_kernel, (n_dev, tokens, model, ffn, n_local, cap)),
            out_shape=[[V(s.shape, s.dtype) for s in saved + saved], V(part.shape, F32), V(part.shape, BF16)] + [V(part.shape, F32)] * 3,
            in_specs=[hbm] * 15,
            out_specs=[[vm] * 10, vm, vm, vm, vm, vm],
            scratch_shapes=scratch,
            compiler_params=pltpu.CompilerParams(collective_id=0, has_side_effects=True, vmem_limit_bytes=MAIN_VMEM),
            name="moe_main",
        )(x, y, dy, experts_one.T, gates_one.T, slots_one.T, experts_two.T, gates_two.T, slots_two.T, wg1, wu1, wd1, wg2, wu2, wd2)

        def shift(v, by):
            return lax.ppermute(v, "expert", [(i, (i + by) % n_dev) for i in range(n_dev)])

        from_left, from_right, from_far = shift(q_right, 2), shift(q_left, n_dev - 2), shift(q_far, n_dev // 2)

        up, down = S((n_local, model, ffn), F32), S((n_local, ffn, model), F32)
        flops = 2 * 2 * n_local * er * model * ffn * 3
        grads = pl.pallas_call(
            functools.partial(grad_kernel, n_local),
            out_shape=[up, up, down] * 2,
            in_specs=[vm] * 10,
            out_specs=[hbm] * 6,
            scratch_shapes=[
                [V((2, model, ffn), F32), V((2, model, ffn), F32), V((2, ffn, model), F32)],
                pltpu.SemaphoreType.DMA((3, 2))],
            compiler_params=pltpu.CompilerParams(vmem_limit_bytes=GRAD_VMEM),
            cost_estimate=pl.CostEstimate(flops=flops, bytes_accessed=6 * n_local * model * ffn * 4, transcendentals=0),
            name="moe_grads",
        )(*kept)
        dx = (dmid.astype(F32) + ((own + from_far) + (from_left + from_right))).astype(BF16)
        return (dx,) + tuple(grads[3:]) + tuple(grads[:3])

    return jax.shard_map(local_step, mesh=mesh, in_specs=(tok_spec,) * 9 + (weight_spec,) * 6, out_specs=(tok_spec,) + (grad_spec,) * 6, check_vma=False)
```

```python
import functools
import jax
import jax.numpy as jnp
from jax import lax
from jax.experimental import pallas as pl
from jax.experimental.pallas import tpu as pltpu
from jax.sharding import PartitionSpec as P

MESH = pl.DeviceIdType.MESH
F32 = jnp.float32
BF16 = jnp.bfloat16
NT = (((1,), (1,)), ((), ()))
TN = (((0,), (0,)), ((), ()))
CHUNKS = 4
DIRECT = 1
COPIES = 41
MAIN_VMEM = 50 * 2**20
GRAD_VMEM = 24 * 2**20


def dot(a, b, dims=(((1,), (0,)), ((), ()))):
    return lax.dot_general(a, b, dims, preferred_element_type=F32)


def slot_capacity(tokens_dev, top_k, n_experts):
    return 8 * ((3 * top_k * tokens_dev + 16 * n_experts - 1) // (16 * n_experts))


def scoped(name):
    def deco(fn):
        def run(*args, **kw):
            tag = "_".join([name] + [str(getattr(a, "tag", a)) for a in args if isinstance(a, (int, Gather))])
            with jax.named_scope(tag):
                return fn(*args, **kw)
        return run
    return deco


class Link:
    def __init__(self, send, recv, partner):
        self.send, self.recv, self.partner, self.used, self.sent = send, recv, partner, 0, []

    def new_set(self, sent):
        self.sent.append(sent)

    def copy(self, src, dst, device, k):
        return pltpu.make_async_remote_copy(
            src_ref=src, dst_ref=dst, send_sem=self.send.at[len(self.sent) - 1], recv_sem=self.recv.at[k],
            device_id={"expert": device}, device_id_type=MESH)

    def whole(self, ref, i, k):
        return pltpu.make_async_remote_copy(
            src_ref=ref, dst_ref=ref, send_sem=self.send.at[i], recv_sem=self.recv.at[k],
            device_id={"expert": self.partner}, device_id_type=MESH)

    def arrived(self, ref, k):
        self.whole(ref, 0, k).wait_recv()

    @scoped("drain")
    def drain(self):
        for i, ref in enumerate(self.sent):
            self.whole(ref, i, 0).wait_send()


class Gather:
    def __init__(self, link, place, own, buf, split, tag, direct=False):
        me, partner, left, right, far = place
        self.link, self.tag, self.direct, self.buf, self.base = link, tag, direct, buf, link.used
        link.used += 5
        link.new_set(buf.at[pl.ds(0, 7)])
        first, second, relay, near, opposite = range(self.base, self.base + 5)
        half = own.shape[0] // 2
        a, b = pl.ds(0, half), pl.ds(half, half)
        self.pair = link.copy(own, buf.at[me], partner, near)
        if direct:
            self.first = [link.copy(own, buf.at[me], right, first), link.copy(own, buf.at[me], left, first)]
            self.second = []
            self.relay = [link.copy(own, buf.at[me], far, relay)]
        else:
            self.first = [link.copy(own.at[a], buf.at[me, a], right, first), link.copy(own.at[b], buf.at[me, b], left, first)]
            self.second = [link.copy(own.at[b], buf.at[me, b], right, second), link.copy(own.at[a], buf.at[me, a], left, second)]
            self.relay = [link.copy(buf.at[left, a], buf.at[left, a], right, relay), link.copy(buf.at[right, b], buf.at[right, b], left, relay)]
        self.near_pair = [link.copy(buf.at[left], buf.at[left], partner, near), link.copy(buf.at[right], buf.at[right], partner, near)]
        self.far_pair = link.copy(buf.at[far], buf.at[far], partner, opposite)

    def arrived(self, which, blocks):
        self.link.arrived(self.buf.at[pl.ds(0, blocks)], self.base + which)

    @scoped("ag_begin")
    def begin(self):
        self.begin_first()
        self.begin_rest()

    def begin_first(self):
        for c in (self.relay if self.direct else []) + self.first:
            c.start()

    def begin_rest(self):
        for c in self.second + [self.pair]:
            c.start()

    @scoped("ag_forward")
    def forward(self):
        self.arrived(0, 2 if self.direct else 1)
        for c in [] if self.direct else self.relay:
            c.start()

    @scoped("ag_share_near")
    def share_near(self):
        if self.second:
            self.arrived(1, 1)
        for c in self.near_pair:
            c.start()

    @scoped("ag_share_far")
    def share_far(self):
        self.arrived(2, 1)
        self.far_pair.start()

    @scoped("ag_finish_near")
    def finish_near(self):
        self.arrived(3, 3)

    @scoped("ag_finish_far")
    def finish_far(self):
        self.arrived(4, 1)


def main_kernel(dims, x_in, y_in, dy_in, e1_in, g1_in, s1_in, e2_in, g2_in, s2_in, wg1, wu1, wd1, wg2, wu2, wd2,
                saved, own_o, dmid_o, qr_o, ql_o, qf_o,
                tok, route, gate, wv, rt, rtg, yg, gg, xg, dg, oh, ot, grow, act_a, act_b, dhp, dxb,
                d1own, q, sd, rd, ra, rb, fl, fr, send, recv, isem, wsem):
    n_dev, tokens, model, ffn, n_local, cap = dims
    n_chips = n_dev // 2
    me = lax.axis_index("expert")
    chip, core = me // 2, lax.rem(me, 2)
    partner = chip * 2 + 1 - core
    right = lax.rem(chip + 1, n_chips) * 2 + core
    left = lax.rem(chip + n_chips - 1, n_chips) * 2 + core
    far = lax.rem(chip + 2, n_chips) * 2 + core
    place = (me, partner, left, right, far)
    rows_chip = 2 * cap
    rows = n_local * rows_chip
    cw = model // CHUNKS
    half = tokens // 2
    u, z, h, da, db = ([saved[i], saved[5 + i]] for i in range(5))

    barrier = pltpu.get_barrier_semaphore()
    for d in (partner, left, right, far):
        pl.semaphore_signal(barrier, inc=1, device_id={"expert": d}, device_id_type=MESH)

    x_ref, y_ref, dy_ref = tok
    hw = model // 2
    e1, s1, e2, s2 = route
    g1, g2 = gate
    loads = []
    for i, (r, v) in enumerate(((y_in, y_ref), (e1_in, e1), (g1_in, g1), (s1_in, s1), (e2_in, e2), (g2_in, g2), (s2_in, s2), (x_in, x_ref), (dy_in.at[:, 0:hw], dy_ref.at[0]), (dy_in.at[:, hw:], dy_ref.at[1]))):
        c = pltpu.make_async_copy(r, v, isem.at[i])
        c.start()
        loads.append(c)
    w_a, w_b, w_c, w_d, w_e, w_f = wv
    wload = {}

    def load(name, src, dst):
        wload[name] = pltpu.make_async_copy(src, dst, wsem.at[len(wload)])
        wload[name].start()

    def need(*names):
        with jax.named_scope("wload"):
            for name in names:
                wload.pop(name).wait()
                wload[name + " done"] = None


    top_k = e1.shape[0]
    link = Link(send, recv, partner)
    g_rt = Gather(link, place, rt, rtg, False, "rt", direct=True)
    g_y = Gather(link, place, y_ref, yg, True, "y")
    g_g = [Gather(link, place, dy_ref.at[i], gg.at[i], True, f"g{i}") for i in range(2)]
    g_x = Gather(link, place, x_ref, xg, True, "x")
    loads[0].wait()
    with jax.named_scope("barrier"):
        pl.semaphore_wait(barrier, 4)

    @scoped("build")
    def build(layer):
        lane = lax.broadcasted_iota(jnp.int32, (top_k, 2 * tokens), 1)
        rid = lax.broadcasted_iota(jnp.int32, (rows, 2 * tokens), 0).astype(F32)
        base = (me * (n_local * rows_chip)).astype(F32)

        def one(c, carry):
            r0, r1 = rtg[2 * c], rtg[2 * c + 1]

            def pick(lo):
                p0, p1 = r0[lo:lo + top_k], r1[lo:lo + top_k]
                if layer == 0:
                    return jnp.where(lane < tokens, p0, pltpu.roll(p1, tokens, 1))
                return jnp.where(lane < tokens, pltpu.roll(p0, tokens, 1), p1)

            t, g = pick(0) - base, pick(top_k)
            hit = jnp.zeros((rows, 2 * tokens), F32)
            gm = jnp.zeros((rows, 2 * tokens), F32)
            for j in range(top_k):
                m = t[j:j + 1] == rid
                hit = jnp.where(m, 1.0, hit)
                gm = jnp.where(m, g[j:j + 1], gm)
            oh[layer, c] = hit.astype(BF16)
            ot[layer, c] = hit.T.astype(BF16)
            grow[layer, c] = jnp.sum(gm, axis=1, keepdims=True)
            return carry

        lax.fori_loop(0, n_chips, one, 0)

    near_chips, far_chip = (chip, left // 2, right // 2), (far // 2,)

    @scoped("rows_of")
    def rows_of(layer, buf, dst, gated, lo, width, chips):
        for c in chips:
            src = jnp.concatenate([buf[2 * c], buf[2 * c + 1]], axis=0)
            r = dot(oh[layer, c], src)
            if gated:
                r = r * grow[layer, c]
            r = r.astype(BF16)
            for e in range(n_local):
                dst[e, pl.ds(pl.multiple_of(c * rows_chip, 16), rows_chip), lo:lo + width] = r[e * rows_chip:(e + 1) * rows_chip]

    @scoped("forward_act")
    def forward_act(layer, e):
        ue = u[layer][e]
        aw = dot(ue, w_a[e]).astype(BF16).astype(F32)
        bw = dot(ue, w_b[e]).astype(BF16).astype(F32)
        sig = jax.nn.sigmoid(aw)
        silu = aw * sig
        h[layer][e] = (silu * bw).astype(BF16)
        act_a[e] = bw * sig * (1.0 + aw * (1.0 - sig))
        act_b[e] = silu

    @scoped("back_part")
    def back_part(layer, width):
        for e in range(n_local):
            dhp[e] = dot(z[layer][e, :, :width], w_d[e, :width])

    @scoped("back_act")
    def back_act(layer, lo):
        for e in range(n_local):
            dh = dot(z[layer][e, :, lo:], w_d[e, lo:])
            if lo:
                dh = dh + dhp[e]
            da[layer][e] = (dh * act_a[e]).astype(BF16)
            db[layer][e] = (dh * act_b[e]).astype(BF16)

    @scoped("flip")
    def flip(src, dst, lo=0, hi=n_local):
        def body(e, carry):
            dst[e] = src[e].T
            return carry
        lax.fori_loop(lo, hi, body, 0)

    gate_t, up_t = (w_c, w_f), (w_e, w_c)

    @scoped("dx_chunk")
    def dx_chunk(layer, k):
        cols = slice(k * cw, (k + 1) * cw)
        for e in range(n_local):
            d = dot(da[layer][e], gate_t[layer][e, :, cols]) + dot(db[layer][e], up_t[layer][e, :, cols])
            d = d.astype(BF16)
            for c in range(n_chips):
                dxb[k, c, e * rows_chip:(e + 1) * rows_chip] = d[c * rows_chip:(c + 1) * rows_chip]
        for c in range(n_chips):
            q[layer, k, c] = dot(ot[layer, c], dxb[k, c])
        for c in pair[layer, k, 0] + pair[layer, k, 1]:
            c.start()

    mine, theirs = pl.multiple_of(core * tokens, tokens), pl.multiple_of((1 - core) * tokens, tokens)

    pair, rs_far, rs_near, base = {}, [], [], link.used
    for k in range(CHUNKS):
        link.new_set(q.at[0, k, :, pl.ds(0, 7 * tokens // n_chips)])
        for i, chips in enumerate((far_chip, near_chips)):
            pair[0, k, i] = [link.copy(q.at[0, k, c, pl.ds(theirs, tokens)], rd.at[0, k, c], partner, base + 4 * k + i) for c in chips]
        rs_far.append([link.copy(sd.at[k, far // 2, pl.ds(0, half)], ra.at[k], right, base + 4 * k + 2),
                       link.copy(sd.at[k, far // 2, pl.ds(half, half)], rb.at[k], left, base + 4 * k + 2)])
        rs_near.append([link.copy(sd.at[k, right // 2], fl.at[k], right, base + 4 * k + 3),
                        link.copy(sd.at[k, left // 2], fr.at[k], left, base + 4 * k + 3)])
    link.new_set(rd.at[1])
    for k in range(CHUNKS):
        pair[1, k, 0] = []
        pair[1, k, 1] = [link.copy(q.at[1, k, :, pl.ds(theirs, tokens)], rd.at[1, k], partner, base + 4 * k + 1)]
    link.used = 0
    ag = [Gather(link, place, d1own.at[k], dg.at[k], True, k, direct=k >= CHUNKS - DIRECT) for k in range(CHUNKS)]

    @scoped("stage_far")
    def stage_far(k):
        link.arrived(fl.at[k], base + 4 * k)
        sd[k, far // 2] = q[0, k, far // 2, pl.ds(mine, tokens)] + rd[0, k, far // 2]
        for c in rs_far[k]:
            c.start()

    @scoped("stage_near")
    def stage_near(k):
        link.arrived(fl.at[k], base + 4 * k + 2)
        link.arrived(sd.at[k, pl.ds(0, 3)], base + 4 * k + 1)
        for c in near_chips:
            sd[k, c] = q[0, k, c, pl.ds(mine, tokens)] + rd[0, k, c]
        sd[k, right // 2, 0:half] = sd[k, right // 2, 0:half] + ra[k]
        sd[k, left // 2, half:] = sd[k, left // 2, half:] + rb[k]
        for c in rs_near[k]:
            c.start()

    @scoped("stage_sum")
    def stage_sum(k):
        link.arrived(sd.at[k, pl.ds(0, 2)], base + 4 * k + 3)
        total = sd[k, chip] + (fl[k] + fr[k])
        d = (dy_ref[k * cw // hw, :, k * cw % hw:k * cw % hw + cw].astype(F32) + total).astype(BF16)
        d1own[k] = d
        dg[k, me] = d
        dmid_o[:, k * cw:(k + 1) * cw] = d
        ag[k].begin()

    @scoped("stage_out")
    def stage_out(k):
        pair[1, k, 1][0].wait_recv()
        cols = slice(k * cw, (k + 1) * cw)
        for c, o in ((chip, own_o), (right // 2, qr_o), (left // 2, ql_o), (far // 2, qf_o)):
            o[:, cols] = q[1, k, c, pl.ds(mine, tokens)] + rd[1, k, c]

    def z_chunk(k):
        ag[k].finish_near()
        ag[k].finish_far()
        rows_of(1, dg.at[k], z[1], True, k * cw, cw, near_chips + far_chip)

    g_y.begin_first()
    for c in loads[1:]:
        c.wait()
    load("down2", wd2, w_c)
    load("gate2", wg2, w_a)
    load("up2", wu2, w_b)
    load("down1", wd1, w_f)
    def target(experts, slots):
        return jnp.where(slots >= 0, experts * rows_chip + core * cap + slots, -1).astype(F32)

    rt[0:top_k, 0:tokens] = target(e2[...], s2[...])
    rt[0:top_k, tokens:2 * tokens] = target(e1[...], s1[...])
    rt[top_k:2 * top_k, 0:tokens] = g2[...]
    rt[top_k:2 * top_k, tokens:2 * tokens] = g1[...]

    g_rt.begin()
    g_y.begin_rest()
    g_g[0].begin()
    rtg[me] = rt[...]
    yg[me] = y_ref[...]
    xg[me] = x_ref[...]
    for i in range(2):
        gg[i, me] = dy_ref[i]
    need("down2")
    flip(w_c, w_d)
    g_rt.forward()
    g_rt.share_near()
    g_y.forward()
    g_g[1].begin()
    g_rt.share_far()
    need("gate2")
    flip(w_a, w_c)
    g_y.share_near()
    g_rt.finish_near()
    g_rt.finish_far()
    build(0)
    g_g[0].forward()
    need("up2")
    flip(w_b, w_e, 0, 2)
    g_y.finish_near()
    rows_of(0, yg, u[0], False, 0, model, near_chips)
    g_y.share_far()
    g_g[1].forward()
    g_x.begin()
    g_g[0].share_near()
    flip(w_b, w_e, 2, 4)
    g_y.finish_far()
    rows_of(0, yg, u[0], False, 0, model, far_chip)
    forward_act(0, 0)
    g_g[1].share_near()
    forward_act(0, 1)
    g_g[0].share_far()
    g_g[0].finish_near()
    rows_of(0, gg.at[0], z[0], True, 0, hw, near_chips)
    forward_act(0, 2)
    g_g[1].share_far()
    g_g[1].finish_near()
    rows_of(0, gg.at[1], z[0], True, hw, hw, near_chips)
    forward_act(0, 3)
    load("gate1", wg1, w_a)
    load("up1", wu1, w_b)
    g_g[0].finish_far()
    rows_of(0, gg.at[0], z[0], True, 0, hw, far_chip)
    back_part(0, hw)
    g_g[1].finish_far()
    rows_of(0, gg.at[1], z[0], True, hw, hw, far_chip)
    back_act(0, hw)
    g_x.forward()

    for k in range(CHUNKS):
        dx_chunk(0, k)
        if k == 0:
            g_x.share_near()
        if k >= 1:
            stage_far(k - 1)
    need("down1")
    flip(w_f, w_d, 0, 2)
    stage_far(CHUNKS - 1)
    g_x.share_far()
    flip(w_f, w_d, 2, 4)
    stage_near(0)
    g_x.finish_near()
    g_x.finish_far()
    build(1)
    stage_near(1)
    rows_of(1, xg, u[1], False, 0, model, near_chips + far_chip)
    stage_near(2)
    need("gate1", "up1")
    forward_act(1, 0)
    stage_near(3)
    flip(w_b, w_c, 0, 4)
    stage_sum(0)
    forward_act(1, 1)
    forward_act(1, 2)
    stage_sum(1)
    forward_act(1, 3)
    flip(w_a, w_f, 0, 2)
    stage_sum(2)
    flip(w_a, w_f, 2, 4)
    stage_sum(3)
    ag[0].forward()
    ag[1].forward()
    ag[0].share_near()
    ag[1].share_near()
    ag[2].forward()
    ag[2].share_near()
    ag[0].share_far()
    ag[3].forward()
    ag[3].share_near()
    ag[1].share_far()
    ag[2].share_far()
    ag[3].share_far()
    z_chunk(0)
    z_chunk(1)
    back_part(1, hw)
    z_chunk(2)
    z_chunk(3)

    back_act(1, hw)
    for k in range(CHUNKS):
        dx_chunk(1, k)
        if k >= 2:
            stage_out(k - 2)
    stage_out(CHUNKS - 2)
    stage_out(CHUNKS - 1)

    link.drain()


def grad_kernel(n_local, *refs):
    ins, outs = refs[:10], refs[10:16]
    vout, osem = refs[16:]

    def store(i, layer, e, s):
        return pltpu.make_async_copy(vout[i].at[s], outs[3 * layer + i].at[e], osem.at[i, s])

    def store_half(i, layer, e, s, part):
        return pltpu.make_async_copy(vout[i].at[s, part], outs[3 * layer + i].at[e, part], osem.at[i, s])

    for layer in range(2):
        u, z, h, da, db = ins[5 * layer:5 * layer + 5]

        def body(e, carry, layer=layer, u=u, z=z, h=h, da=da, db=db):
            s = lax.rem(e, 2)
            for i, (a, b) in enumerate(((u, da), (u, db), (h, z))):
                def reclaim(i=i):
                    store(i, layer, e, s).wait()

                if layer == 0:
                    pl.when(e >= 2)(reclaim)
                else:
                    reclaim()
                n = a.shape[2] // 2
                for p in range(2):
                    vout[i][s, p * n:(p + 1) * n] = dot(a[e, :, p * n:(p + 1) * n], b[e], TN)
                    store_half(i, layer, e, s, pl.ds(p * n, n)).start()
            return carry

        lax.fori_loop(0, n_local, body, 0)
    for s in range(2):
        for i in range(3):
            store(i, 1, n_local - 2 + s, s).wait()


def solution(mesh):
    n_dev = mesh.shape["expert"]
    tok_spec = P(("data", "expert"), None)
    weight_spec = P("expert", None, None)
    grad_spec = P(("data", "expert"), None, None)

    def local_step(x, y, dy, experts_one, gates_one, slots_one, experts_two, gates_two, slots_two, wg1, wu1, wd1, wg2, wu2, wd2):
        tokens, model = x.shape
        n_local, _, ffn = wg1.shape
        top_k = experts_one.shape[1]
        cap = slot_capacity(tokens, top_k, n_local * n_dev)
        n_chips = n_dev // 2
        rows = n_local * 2 * cap
        cw = model // CHUNKS
        half = tokens // 2

        S = jax.ShapeDtypeStruct
        er = n_chips * 2 * cap
        wide, narrow = S((n_local, er, model), BF16), S((n_local, er, ffn), BF16)
        saved = [wide, wide, narrow, narrow, narrow]
        part = S((tokens, model), F32)
        hbm, vm = pl.BlockSpec(memory_space=pltpu.HBM), pl.BlockSpec(memory_space=pltpu.VMEM)
        V = pltpu.VMEM
        scratch = [
            [V((tokens, model), BF16), V((tokens, model), BF16), V((2, tokens, model // 2), BF16)], [V((top_k, tokens), jnp.int32)] * 4, [V((top_k, tokens), F32)] * 2,
            [V(w.shape, BF16) for w in (wg2, wg2, wd2, wg2, wd2, wd2)],
            V((2 * top_k, 2 * tokens), F32), V((n_dev, 2 * top_k, 2 * tokens), F32),
            V((n_dev, tokens, model), BF16), V((2, n_dev, tokens, model // 2), BF16), V((n_dev, tokens, model), BF16),
            V((CHUNKS, n_dev, tokens, cw), BF16),
            V((2, n_chips, rows, 2 * tokens), BF16), V((2, n_chips, 2 * tokens, rows), BF16), V((2, n_chips, rows, 1), F32),
            V((n_local, er, ffn), F32), V((n_local, er, ffn), F32), V((n_local, er, ffn), F32),
            V((CHUNKS, n_chips, rows, cw), BF16),
            V((CHUNKS, tokens, cw), BF16),
            V((2, CHUNKS, n_chips, 2 * tokens, cw), F32),
            V((CHUNKS, n_chips, tokens, cw), F32),
            V((2, CHUNKS, n_chips, tokens, cw), F32),
            V((CHUNKS, half, cw), F32), V((CHUNKS, half, cw), F32),
            V((CHUNKS, tokens, cw), F32), V((CHUNKS, tokens, cw), F32),
            pltpu.SemaphoreType.DMA((10 + CHUNKS,)), pltpu.SemaphoreType.DMA((COPIES,)),
            pltpu.SemaphoreType.DMA((10,)), pltpu.SemaphoreType.DMA((6,)),
        ]
        kept, own, dmid, q_right, q_left, q_far = pl.pallas_call(
            functools.partial(main_kernel, (n_dev, tokens, model, ffn, n_local, cap)),
            out_shape=[[V(s.shape, s.dtype) for s in saved + saved], V(part.shape, F32), V(part.shape, BF16)] + [V(part.shape, F32)] * 3,
            in_specs=[hbm] * 15,
            out_specs=[[vm] * 10, vm, vm, vm, vm, vm],
            scratch_shapes=scratch,
            compiler_params=pltpu.CompilerParams(collective_id=0, has_side_effects=True, vmem_limit_bytes=MAIN_VMEM),
            name="moe_main",
        )(x, y, dy, experts_one.T, gates_one.T, slots_one.T, experts_two.T, gates_two.T, slots_two.T, wg1, wu1, wd1, wg2, wu2, wd2)

        def shift(v, by):
            return lax.ppermute(v, "expert", [(i, (i + by) % n_dev) for i in range(n_dev)])

        from_left, from_right, from_far = shift(q_right, 2), shift(q_left, n_dev - 2), shift(q_far, n_dev // 2)

        up, down = S((n_local, model, ffn), F32), S((n_local, ffn, model), F32)
        flops = 2 * 2 * n_local * er * model * ffn * 3
        grads = pl.pallas_call(
            functools.partial(grad_kernel, n_local),
            out_shape=[up, up, down] * 2,
            in_specs=[vm] * 10,
            out_specs=[hbm] * 6,
            scratch_shapes=[
                [V((2, model, ffn), F32), V((2, model, ffn), F32), V((2, ffn, model), F32)],
                pltpu.SemaphoreType.DMA((3, 2))],
            compiler_params=pltpu.CompilerParams(vmem_limit_bytes=GRAD_VMEM),
            cost_estimate=pl.CostEstimate(flops=flops, bytes_accessed=6 * n_local * model * ffn * 4, transcendentals=0),
            name="moe_grads",
        )(*kept)
        dx = (dmid.astype(F32) + ((own + from_far) + (from_left + from_right))).astype(BF16)
        return (dx,) + tuple(grads[3:]) + tuple(grads[:3])

    return jax.shard_map(local_step, mesh=mesh, in_specs=(tok_spec,) * 9 + (weight_spec,) * 6, out_specs=(tok_spec,) + (grad_spec,) * 6, check_vma=False)
```

```python
import functools
import jax
import jax.numpy as jnp
from jax import lax
from jax.experimental import pallas as pl
from jax.experimental.pallas import tpu as pltpu
from jax.sharding import PartitionSpec as P

MESH = pl.DeviceIdType.MESH
F32 = jnp.float32
BF16 = jnp.bfloat16
NT = (((1,), (1,)), ((), ()))
TN = (((0,), (0,)), ((), ()))
CHUNKS = 4
DIRECT = 1
COPIES = 41
MAIN_VMEM = 50 * 2**20
GRAD_VMEM = 24 * 2**20


def dot(a, b, dims=(((1,), (0,)), ((), ()))):
    return lax.dot_general(a, b, dims, preferred_element_type=F32)


def slot_capacity(tokens_dev, top_k, n_experts):
    return 8 * ((3 * top_k * tokens_dev + 16 * n_experts - 1) // (16 * n_experts))


def scoped(name):
    def deco(fn):
        def run(*args, **kw):
            tag = "_".join([name] + [str(getattr(a, "tag", a)) for a in args if isinstance(a, (int, Gather))])
            with jax.named_scope(tag):
                return fn(*args, **kw)
        return run
    return deco


class Link:
    def __init__(self, send, recv, partner):
        self.send, self.recv, self.partner, self.used, self.sent = send, recv, partner, 0, []

    def new_set(self, sent):
        self.sent.append(sent)

    def copy(self, src, dst, device, k):
        return pltpu.make_async_remote_copy(
            src_ref=src, dst_ref=dst, send_sem=self.send.at[len(self.sent) - 1], recv_sem=self.recv.at[k],
            device_id={"expert": device}, device_id_type=MESH)

    def whole(self, ref, i, k):
        return pltpu.make_async_remote_copy(
            src_ref=ref, dst_ref=ref, send_sem=self.send.at[i], recv_sem=self.recv.at[k],
            device_id={"expert": self.partner}, device_id_type=MESH)

    def arrived(self, ref, k):
        self.whole(ref, 0, k).wait_recv()

    @scoped("drain")
    def drain(self):
        for i, ref in enumerate(self.sent):
            self.whole(ref, i, 0).wait_send()


class Gather:
    def __init__(self, link, place, own, buf, split, tag, direct=False):
        me, partner, left, right, far = place
        self.link, self.tag, self.direct, self.buf, self.base = link, tag, direct, buf, link.used
        link.used += 5
        link.new_set(buf.at[pl.ds(0, 7)])
        first, second, relay, near, opposite = range(self.base, self.base + 5)
        half = own.shape[0] // 2
        a, b = pl.ds(0, half), pl.ds(half, half)
        self.pair = link.copy(own, buf.at[me], partner, near)
        if direct:
            self.first = [link.copy(own, buf.at[me], right, first), link.copy(own, buf.at[me], left, first)]
            self.second = []
            self.relay = [link.copy(own, buf.at[me], far, relay)]
        else:
            self.first = [link.copy(own.at[a], buf.at[me, a], right, first), link.copy(own.at[b], buf.at[me, b], left, first)]
            self.second = [link.copy(own.at[b], buf.at[me, b], right, second), link.copy(own.at[a], buf.at[me, a], left, second)]
            self.relay = [link.copy(buf.at[left, a], buf.at[left, a], right, relay), link.copy(buf.at[right, b], buf.at[right, b], left, relay)]
        self.near_pair = [link.copy(buf.at[left], buf.at[left], partner, near), link.copy(buf.at[right], buf.at[right], partner, near)]
        self.far_pair = link.copy(buf.at[far], buf.at[far], partner, opposite)

    def arrived(self, which, blocks):
        self.link.arrived(self.buf.at[pl.ds(0, blocks)], self.base + which)

    @scoped("ag_begin")
    def begin(self):
        self.begin_first()
        self.begin_rest()

    def begin_first(self):
        for c in (self.relay if self.direct else []) + self.first:
            c.start()

    def begin_rest(self):
        for c in self.second + [self.pair]:
            c.start()

    @scoped("ag_forward")
    def forward(self):
        self.arrived(0, 2 if self.direct else 1)
        for c in [] if self.direct else self.relay:
            c.start()

    @scoped("ag_share_near")
    def share_near(self):
        if self.second:
            self.arrived(1, 1)
        for c in self.near_pair:
            c.start()

    @scoped("ag_share_far")
    def share_far(self):
        self.arrived(2, 1)
        self.far_pair.start()

    @scoped("ag_finish_near")
    def finish_near(self):
        self.arrived(3, 3)

    @scoped("ag_finish_far")
    def finish_far(self):
        self.arrived(4, 1)


def main_kernel(dims, x_in, y_in, dy_in, e1_in, g1_in, s1_in, e2_in, g2_in, s2_in, wg1, wu1, wd1, wg2, wu2, wd2,
                saved, own_o, qr_o, ql_o, qf_o,
                tok, route, gate, wv, rt, rtg, yg, gg, xg, dg, oh, ot, grow, act_a, act_b, dhp, dxb,
                d1own, q, sd, rd, ra, rb, fl, fr, send, recv, isem, wsem):
    n_dev, tokens, model, ffn, n_local, cap = dims
    n_chips = n_dev // 2
    me = lax.axis_index("expert")
    chip, core = me // 2, lax.rem(me, 2)
    partner = chip * 2 + 1 - core
    right = lax.rem(chip + 1, n_chips) * 2 + core
    left = lax.rem(chip + n_chips - 1, n_chips) * 2 + core
    far = lax.rem(chip + 2, n_chips) * 2 + core
    place = (me, partner, left, right, far)
    rows_chip = 2 * cap
    rows = n_local * rows_chip
    cw = model // CHUNKS
    half = tokens // 2
    u, z, h, da, db = ([saved[i], saved[5 + i]] for i in range(5))

    barrier = pltpu.get_barrier_semaphore()
    for d in (partner, left, right, far):
        pl.semaphore_signal(barrier, inc=1, device_id={"expert": d}, device_id_type=MESH)

    x_ref, y_ref, dy_ref = tok
    hw = model // 2
    e1, s1, e2, s2 = route
    g1, g2 = gate
    loads = []
    for i, (r, v) in enumerate(((y_in, y_ref), (e1_in, e1), (g1_in, g1), (s1_in, s1), (e2_in, e2), (g2_in, g2), (s2_in, s2), (x_in, x_ref), (dy_in.at[:, 0:hw], dy_ref.at[0]), (dy_in.at[:, hw:], dy_ref.at[1]))):
        c = pltpu.make_async_copy(r, v, isem.at[i])
        c.start()
        loads.append(c)
    w_a, w_b, w_c, w_d, w_e, w_f = wv
    wload = {}

    def load(name, src, dst):
        wload[name] = pltpu.make_async_copy(src, dst, wsem.at[len(wload)])
        wload[name].start()

    def need(*names):
        with jax.named_scope("wload"):
            for name in names:
                wload.pop(name).wait()
                wload[name + " done"] = None


    top_k = e1.shape[0]
    link = Link(send, recv, partner)
    g_rt = Gather(link, place, rt, rtg, False, "rt", direct=True)
    g_y = Gather(link, place, y_ref, yg, True, "y")
    g_g = [Gather(link, place, dy_ref.at[i], gg.at[i], True, f"g{i}") for i in range(2)]
    g_x = Gather(link, place, x_ref, xg, True, "x")
    loads[0].wait()
    with jax.named_scope("barrier"):
        pl.semaphore_wait(barrier, 4)

    @scoped("build")
    def build(layer):
        lane = lax.broadcasted_iota(jnp.int32, (top_k, 2 * tokens), 1)
        rid = lax.broadcasted_iota(jnp.int32, (rows, 2 * tokens), 0).astype(F32)
        base = (me * (n_local * rows_chip)).astype(F32)

        def one(c, carry):
            r0, r1 = rtg[2 * c], rtg[2 * c + 1]

            def pick(lo):
                p0, p1 = r0[lo:lo + top_k], r1[lo:lo + top_k]
                if layer == 0:
                    return jnp.where(lane < tokens, p0, pltpu.roll(p1, tokens, 1))
                return jnp.where(lane < tokens, pltpu.roll(p0, tokens, 1), p1)

            t, g = pick(0) - base, pick(top_k)
            hit = jnp.zeros((rows, 2 * tokens), F32)
            gm = jnp.zeros((rows, 2 * tokens), F32)
            for j in range(top_k):
                m = t[j:j + 1] == rid
                hit = jnp.where(m, 1.0, hit)
                gm = jnp.where(m, g[j:j + 1], gm)
            oh[layer, c] = hit.astype(BF16)
            ot[layer, c] = hit.T.astype(BF16)
            grow[layer, c] = jnp.sum(gm, axis=1, keepdims=True)
            return carry

        lax.fori_loop(0, n_chips, one, 0)

    near_chips, far_chip = (chip, left // 2, right // 2), (far // 2,)

    @scoped("rows_of")
    def rows_of(layer, buf, dst, gated, lo, width, chips):
        for c in chips:
            src = jnp.concatenate([buf[2 * c], buf[2 * c + 1]], axis=0)
            r = dot(oh[layer, c], src)
            if gated:
                r = r * grow[layer, c]
            r = r.astype(BF16)
            for e in range(n_local):
                dst[e, pl.ds(pl.multiple_of(c * rows_chip, 16), rows_chip), lo:lo + width] = r[e * rows_chip:(e + 1) * rows_chip]

    @scoped("forward_act")
    def forward_act(layer, e):
        ue = u[layer][e]
        aw = dot(ue, w_a[e]).astype(BF16).astype(F32)
        bw = dot(ue, w_b[e]).astype(BF16).astype(F32)
        sig = jax.nn.sigmoid(aw)
        silu = aw * sig
        h[layer][e] = (silu * bw).astype(BF16)
        act_a[e] = bw * sig * (1.0 + aw * (1.0 - sig))
        act_b[e] = silu

    @scoped("back_part")
    def back_part(layer, width):
        for e in range(n_local):
            dhp[e] = dot(z[layer][e, :, :width], w_d[e, :width])

    @scoped("back_act")
    def back_act(layer, lo):
        for e in range(n_local):
            dh = dot(z[layer][e, :, lo:], w_d[e, lo:])
            if lo:
                dh = dh + dhp[e]
            da[layer][e] = (dh * act_a[e]).astype(BF16)
            db[layer][e] = (dh * act_b[e]).astype(BF16)

    @scoped("flip")
    def flip(src, dst, lo=0, hi=n_local):
        def body(e, carry):
            dst[e] = src[e].T
            return carry
        lax.fori_loop(lo, hi, body, 0)

    gate_t, up_t = (w_c, w_f), (w_e, w_c)

    @scoped("dx_chunk")
    def dx_chunk(layer, k):
        cols = slice(k * cw, (k + 1) * cw)
        for e in range(n_local):
            d = dot(da[layer][e], gate_t[layer][e, :, cols]) + dot(db[layer][e], up_t[layer][e, :, cols])
            d = d.astype(BF16)
            for c in range(n_chips):
                dxb[k, c, e * rows_chip:(e + 1) * rows_chip] = d[c * rows_chip:(c + 1) * rows_chip]
        for c in range(n_chips):
            q[layer, k, c] = dot(ot[layer, c], dxb[k, c])
        for c in pair[layer, k, 0] + pair[layer, k, 1]:
            c.start()

    mine, theirs = pl.multiple_of(core * tokens, tokens), pl.multiple_of((1 - core) * tokens, tokens)

    pair, rs_far, rs_near, base = {}, [], [], link.used
    for k in range(CHUNKS):
        link.new_set(q.at[0, k, :, pl.ds(0, 7 * tokens // n_chips)])
        for i, chips in enumerate((far_chip, near_chips)):
            pair[0, k, i] = [link.copy(q.at[0, k, c, pl.ds(theirs, tokens)], rd.at[0, k, c], partner, base + 4 * k + i) for c in chips]
        rs_far.append([link.copy(sd.at[k, far // 2, pl.ds(0, half)], ra.at[k], right, base + 4 * k + 2),
                       link.copy(sd.at[k, far // 2, pl.ds(half, half)], rb.at[k], left, base + 4 * k + 2)])
        rs_near.append([link.copy(sd.at[k, right // 2], fl.at[k], right, base + 4 * k + 3),
                        link.copy(sd.at[k, left // 2], fr.at[k], left, base + 4 * k + 3)])
    link.new_set(rd.at[1])
    for k in range(CHUNKS):
        pair[1, k, 0] = []
        pair[1, k, 1] = [link.copy(q.at[1, k, :, pl.ds(theirs, tokens)], rd.at[1, k], partner, base + 4 * k + 1)]
    link.used = 0
    ag = [Gather(link, place, d1own.at[k], dg.at[k], True, k, direct=k >= CHUNKS - DIRECT) for k in range(CHUNKS)]

    @scoped("stage_far")
    def stage_far(k):
        link.arrived(fl.at[k], base + 4 * k)
        sd[k, far // 2] = q[0, k, far // 2, pl.ds(mine, tokens)] + rd[0, k, far // 2]
        for c in rs_far[k]:
            c.start()

    @scoped("stage_near")
    def stage_near(k):
        link.arrived(fl.at[k], base + 4 * k + 2)
        link.arrived(sd.at[k, pl.ds(0, 3)], base + 4 * k + 1)
        for c in near_chips:
            sd[k, c] = q[0, k, c, pl.ds(mine, tokens)] + rd[0, k, c]
        sd[k, right // 2, 0:half] = sd[k, right // 2, 0:half] + ra[k]
        sd[k, left // 2, half:] = sd[k, left // 2, half:] + rb[k]
        for c in rs_near[k]:
            c.start()

    @scoped("stage_sum")
    def stage_sum(k):
        link.arrived(sd.at[k, pl.ds(0, 2)], base + 4 * k + 3)
        total = sd[k, chip] + (fl[k] + fr[k])
        d = (dy_ref[k * cw // hw, :, k * cw % hw:k * cw % hw + cw].astype(F32) + total).astype(BF16)
        d1own[k] = d
        dg[k, me] = d
        ag[k].begin()

    @scoped("stage_out")
    def stage_out(k):
        pair[1, k, 1][0].wait_recv()
        cols = slice(k * cw, (k + 1) * cw)
        for c, o in ((chip, own_o), (right // 2, qr_o), (left // 2, ql_o), (far // 2, qf_o)):
            part = q[1, k, c, pl.ds(mine, tokens)] + rd[1, k, c]
            o[:, cols] = part + d1own[k].astype(F32) if o is own_o else part

    def z_chunk(k):
        ag[k].finish_near()
        ag[k].finish_far()
        rows_of(1, dg.at[k], z[1], True, k * cw, cw, near_chips + far_chip)

    g_y.begin_first()
    for c in loads[1:]:
        c.wait()
    load("down2", wd2, w_c)
    load("gate2", wg2, w_a)
    load("up2", wu2, w_b)
    load("down1", wd1, w_f)
    def target(experts, slots):
        return jnp.where(slots >= 0, experts * rows_chip + core * cap + slots, -1).astype(F32)

    rt[0:top_k, 0:tokens] = target(e2[...], s2[...])
    rt[0:top_k, tokens:2 * tokens] = target(e1[...], s1[...])
    rt[top_k:2 * top_k, 0:tokens] = g2[...]
    rt[top_k:2 * top_k, tokens:2 * tokens] = g1[...]

    g_rt.begin()
    g_y.begin_rest()
    g_g[0].begin()
    rtg[me] = rt[...]
    yg[me] = y_ref[...]
    xg[me] = x_ref[...]
    for i in range(2):
        gg[i, me] = dy_ref[i]
    need("down2")
    flip(w_c, w_d)
    g_rt.forward()
    g_rt.share_near()
    g_y.forward()
    g_g[1].begin()
    g_rt.share_far()
    need("gate2")
    flip(w_a, w_c)
    g_y.share_near()
    g_rt.finish_near()
    g_rt.finish_far()
    build(0)
    g_g[0].forward()
    need("up2")
    flip(w_b, w_e, 0, 2)
    g_y.finish_near()
    rows_of(0, yg, u[0], False, 0, model, near_chips)
    g_y.share_far()
    g_g[1].forward()
    g_x.begin()
    g_g[0].share_near()
    flip(w_b, w_e, 2, 4)
    g_y.finish_far()
    rows_of(0, yg, u[0], False, 0, model, far_chip)
    forward_act(0, 0)
    g_g[1].share_near()
    forward_act(0, 1)
    g_g[0].share_far()
    g_g[0].finish_near()
    rows_of(0, gg.at[0], z[0], True, 0, hw, near_chips)
    forward_act(0, 2)
    g_g[1].share_far()
    g_g[1].finish_near()
    rows_of(0, gg.at[1], z[0], True, hw, hw, near_chips)
    forward_act(0, 3)
    load("gate1", wg1, w_a)
    load("up1", wu1, w_b)
    g_g[0].finish_far()
    rows_of(0, gg.at[0], z[0], True, 0, hw, far_chip)
    back_part(0, hw)
    g_g[1].finish_far()
    rows_of(0, gg.at[1], z[0], True, hw, hw, far_chip)
    back_act(0, hw)
    g_x.forward()

    for k in range(CHUNKS):
        dx_chunk(0, k)
        if k == 0:
            g_x.share_near()
        if k >= 1:
            stage_far(k - 1)
    need("down1")
    flip(w_f, w_d, 0, 2)
    stage_far(CHUNKS - 1)
    g_x.share_far()
    flip(w_f, w_d, 2, 4)
    stage_near(0)
    g_x.finish_near()
    g_x.finish_far()
    build(1)
    stage_near(1)
    rows_of(1, xg, u[1], False, 0, model, near_chips + far_chip)
    stage_near(2)
    need("gate1", "up1")
    forward_act(1, 0)
    stage_near(3)
    flip(w_b, w_c, 0, 4)
    stage_sum(0)
    forward_act(1, 1)
    forward_act(1, 2)
    stage_sum(1)
    forward_act(1, 3)
    flip(w_a, w_f, 0, 2)
    stage_sum(2)
    flip(w_a, w_f, 2, 4)
    stage_sum(3)
    ag[0].forward()
    ag[1].forward()
    ag[0].share_near()
    ag[1].share_near()
    ag[2].forward()
    ag[2].share_near()
    ag[0].share_far()
    ag[3].forward()
    ag[3].share_near()
    ag[1].share_far()
    ag[2].share_far()
    ag[3].share_far()
    z_chunk(0)
    z_chunk(1)
    back_part(1, hw)
    z_chunk(2)
    z_chunk(3)

    back_act(1, hw)
    for k in range(CHUNKS):
        dx_chunk(1, k)
        if k >= 2:
            stage_out(k - 2)
    stage_out(CHUNKS - 2)
    stage_out(CHUNKS - 1)

    link.drain()


def grad_kernel(n_local, *refs):
    ins, outs = refs[:10], refs[10:16]
    vout, osem = refs[16:]

    def store(i, layer, e, s):
        return pltpu.make_async_copy(vout[i].at[s], outs[3 * layer + i].at[e], osem.at[i, s])

    def store_half(i, layer, e, s, part):
        return pltpu.make_async_copy(vout[i].at[s, part], outs[3 * layer + i].at[e, part], osem.at[i, s])

    for layer in range(2):
        u, z, h, da, db = ins[5 * layer:5 * layer + 5]

        def body(e, carry, layer=layer, u=u, z=z, h=h, da=da, db=db):
            s = lax.rem(e, 2)
            for i, (a, b) in enumerate(((u, da), (u, db), (h, z))):
                def reclaim(i=i):
                    store(i, layer, e, s).wait()

                if layer == 0:
                    pl.when(e >= 2)(reclaim)
                else:
                    reclaim()
                n = a.shape[2] // 4
                for p in range(4):
                    vout[i][s, p * n:(p + 1) * n] = dot(a[e, :, p * n:(p + 1) * n], b[e], TN)
                    store_half(i, layer, e, s, pl.ds(p * n, n)).start()
            return carry

        lax.fori_loop(0, n_local, body, 0)
    for s in range(2):
        for i in range(3):
            store(i, 1, n_local - 2 + s, s).wait()


def solution(mesh):
    n_dev = mesh.shape["expert"]
    tok_spec = P(("data", "expert"), None)
    weight_spec = P("expert", None, None)
    grad_spec = P(("data", "expert"), None, None)

    def local_step(x, y, dy, experts_one, gates_one, slots_one, experts_two, gates_two, slots_two, wg1, wu1, wd1, wg2, wu2, wd2):
        tokens, model = x.shape
        n_local, _, ffn = wg1.shape
        top_k = experts_one.shape[1]
        cap = slot_capacity(tokens, top_k, n_local * n_dev)
        n_chips = n_dev // 2
        rows = n_local * 2 * cap
        cw = model // CHUNKS
        half = tokens // 2

        S = jax.ShapeDtypeStruct
        er = n_chips * 2 * cap
        wide, narrow = S((n_local, er, model), BF16), S((n_local, er, ffn), BF16)
        saved = [wide, wide, narrow, narrow, narrow]
        part = S((tokens, model), F32)
        hbm, vm = pl.BlockSpec(memory_space=pltpu.HBM), pl.BlockSpec(memory_space=pltpu.VMEM)
        V = pltpu.VMEM
        scratch = [
            [V((tokens, model), BF16), V((tokens, model), BF16), V((2, tokens, model // 2), BF16)], [V((top_k, tokens), jnp.int32)] * 4, [V((top_k, tokens), F32)] * 2,
            [V(w.shape, BF16) for w in (wg2, wg2, wd2, wg2, wd2, wd2)],
            V((2 * top_k, 2 * tokens), F32), V((n_dev, 2 * top_k, 2 * tokens), F32),
            V((n_dev, tokens, model), BF16), V((2, n_dev, tokens, model // 2), BF16), V((n_dev, tokens, model), BF16),
            V((CHUNKS, n_dev, tokens, cw), BF16),
            V((2, n_chips, rows, 2 * tokens), BF16), V((2, n_chips, 2 * tokens, rows), BF16), V((2, n_chips, rows, 1), F32),
            V((n_local, er, ffn), F32), V((n_local, er, ffn), F32), V((n_local, er, ffn), F32),
            V((CHUNKS, n_chips, rows, cw), BF16),
            V((CHUNKS, tokens, cw), BF16),
            V((2, CHUNKS, n_chips, 2 * tokens, cw), F32),
            V((CHUNKS, n_chips, tokens, cw), F32),
            V((2, CHUNKS, n_chips, tokens, cw), F32),
            V((CHUNKS, half, cw), F32), V((CHUNKS, half, cw), F32),
            V((CHUNKS, tokens, cw), F32), V((CHUNKS, tokens, cw), F32),
            pltpu.SemaphoreType.DMA((10 + CHUNKS,)), pltpu.SemaphoreType.DMA((COPIES,)),
            pltpu.SemaphoreType.DMA((10,)), pltpu.SemaphoreType.DMA((6,)),
        ]
        kept, own, q_right, q_left, q_far = pl.pallas_call(
            functools.partial(main_kernel, (n_dev, tokens, model, ffn, n_local, cap)),
            out_shape=[[V(s.shape, s.dtype) for s in saved + saved], V(part.shape, F32)] + [V(part.shape, F32)] * 3,
            in_specs=[hbm] * 15,
            out_specs=[[vm] * 10, vm, vm, vm, vm],
            scratch_shapes=scratch,
            compiler_params=pltpu.CompilerParams(collective_id=0, has_side_effects=True, vmem_limit_bytes=MAIN_VMEM),
            name="moe_main",
        )(x, y, dy, experts_one.T, gates_one.T, slots_one.T, experts_two.T, gates_two.T, slots_two.T, wg1, wu1, wd1, wg2, wu2, wd2)

        def shift(v, by):
            return lax.ppermute(v, "expert", [(i, (i + by) % n_dev) for i in range(n_dev)])

        from_left, from_right, from_far = shift(q_right, 2), shift(q_left, n_dev - 2), shift(q_far, n_dev // 2)

        up, down = S((n_local, model, ffn), F32), S((n_local, ffn, model), F32)
        flops = 2 * 2 * n_local * er * model * ffn * 3
        grads = pl.pallas_call(
            functools.partial(grad_kernel, n_local),
            out_shape=[up, up, down] * 2,
            in_specs=[vm] * 10,
            out_specs=[hbm] * 6,
            scratch_shapes=[
                [V((2, model, ffn), F32), V((2, model, ffn), F32), V((2, ffn, model), F32)],
                pltpu.SemaphoreType.DMA((3, 2))],
            compiler_params=pltpu.CompilerParams(vmem_limit_bytes=GRAD_VMEM),
            cost_estimate=pl.CostEstimate(flops=flops, bytes_accessed=6 * n_local * model * ffn * 4, transcendentals=0),
            name="moe_grads",
        )(*kept)
        dx = ((own + from_far) + (from_left + from_right)).astype(BF16)
        return (dx,) + tuple(grads[3:]) + tuple(grads[:3])

    return jax.shard_map(local_step, mesh=mesh, in_specs=(tok_spec,) * 9 + (weight_spec,) * 6, out_specs=(tok_spec,) + (grad_spec,) * 6, check_vma=False)
```
